128 devices in a mesh: band: 16 (over z, y), chan: 4 (over x), member: 2 (over core).
Axes of the slice: x: 4, y: 4, z: 4, core: 2. Of those that a mesh axis runs over, the one named last changes fastest.
Arguments:
- noisy_state: bfloat16 [8, 84, 32768], P(('chan', 'member'), None, 'band'), may hold values from -6 to 6
- target_state: bfloat16 [8, 84, 32768], P(('chan', 'member'), None, 'band'), may hold values from -6 to 6
- noise_level: float32 [8], P(('chan', 'member')), may hold values from 0.3 to 3
- var_weight: float32 [84], replicated, may hold values from 0.3 to 3
- embed_in: bfloat16 [84, 512], replicated, may hold values from -0.625 to 0.625
- embed_out: bfloat16 [512, 512], replicated, may hold values from -0.25 to 0.25
- norm_gain: float32 [512], replicated, may hold values from 0.1 to 1.9
- qkv_weight: bfloat16 [3, 512, 512], replicated, may hold values from -0.25 to 0.25
- head_scale: float32 [4], replicated, may hold values from 1 to 4
- out_weight: bfloat16 [512, 512], replicated, may hold values from -0.25 to 0.25
- dec_weight: bfloat16 [512, 84], replicated, may hold values from -0.25 to 0.25
- g2m_node: int32 [32768], P('band'), may hold values from 0 to 8191, as said below
- m2g_node: int32 [32768], P('band'), may hold values from 0 to 8191, as said below
- neighbours: int32 [8192, 32], P('band'), may hold values from 0 to 8191, as said below
Outputs:
- loss_value: float32 [], replicated
- grad_dec: float32 [512, 84], replicated
- grad_out: float32 [512, 512], replicated
- grad_value: float32 [512, 512], replicated
The draws below stay inside these ranges and needn't reach their ends.
Inputs may be any that keep to these rules, and one draw needn't show every extreme that they name: `g2m_node`: the node of cell g lies in patch g // 2048 or in a patch next to it; patch p holds the nodes p * 512 to (p + 1) * 512 - 1. `m2g_node`: the node of cell g lies in patch g // 2048 or in a patch next to it; patch p holds the nodes p * 512 to (p + 1) * 512 - 1. The neighbours of node n lie in patch n // 512 or in a patch next to it.
All inputs are finite; a program needn't handle non-finite values.
Results may differ from the reference program's by a relative error of at most 0.0003.
Values may be sent and summed in bfloat16 or wider, within the bound.
A program may use at most 64 MiB of HBM per device.

```python
import math
import jax
import jax.numpy as jnp
from jax import lax

D = 512
VARS = 84
HEADS = 4
NBR = 32
G_DEV = 2048
M_DEV = 512
HEAD_DIM = 128
GRID = 32768
MESH = 8192
MEMBERS = 8


def nearby_nodes(key, patches):
    first_key, second_key = jax.random.split(key)
    offsets = jnp.array([-1, 0, 0, 1], dtype=jnp.int32)
    choose = jax.random.randint(first_key, patches.shape, 0, 4)
    shifted = jnp.clip(patches + offsets[choose], 0, MESH // M_DEV - 1)
    within = jax.random.randint(second_key, patches.shape, 0, M_DEV)
    return (shifted * M_DEV + within).astype(jnp.int32)


def draw_g2m_node(key, part):
    patches = jnp.arange(GRID, dtype=jnp.int32) // G_DEV
    return nearby_nodes(jax.random.fold_in(key, 101), patches)


def draw_m2g_node(key, part):
    patches = jnp.arange(GRID, dtype=jnp.int32) // G_DEV
    return nearby_nodes(jax.random.fold_in(key, 202), patches)


def draw_neighbours(key, part):
    patches = jnp.broadcast_to((jnp.arange(MESH, dtype=jnp.int32) // M_DEV)[:, None], (MESH, NBR))
    return nearby_nodes(jax.random.fold_in(key, 303), patches)


def level_of(key, extent, cuts, smallest, top_value):
    level = 1.0
    for dim, blocks in cuts:
        draws = jax.random.uniform(jax.random.fold_in(jax.random.fold_in(key, 6), dim), (blocks,), jnp.float32, smallest / len(cuts), top_value / len(cuts))
        level = level * jnp.repeat(jnp.exp(draws), extent[dim] // blocks).reshape((-1,) + (1,) * (len(extent) - 1 - dim))
    return level


def normal_values(stream_key, extent, scale, reach, pieces=(), kind=jnp.bfloat16):
    drawn = jax.random.normal(stream_key, extent, jnp.float32) * scale
    if len(pieces) > 0:
        drawn = level_of(stream_key, extent, pieces, -0.22, 0.18) * drawn
    return jnp.clip(drawn, min=-reach, max=reach).astype(kind)


def setup_inputs(seed: int = 0) -> dict:
    keys = jax.random.split(jax.random.key(seed), 15)
    return {
        "noisy_state": normal_values(keys[0], (MEMBERS, VARS, GRID), 1.0, 6.0, ((0, 8), (2, 16))),
        "target_state": normal_values(keys[1], (MEMBERS, VARS, GRID), 1.0, 6.0, ((0, 8), (2, 16))),
        "noise_level": jnp.clip(jnp.exp(math.log(3.0) - 2.3025851 * jax.random.uniform(keys[2], (MEMBERS,), jnp.float32) ** level_of(keys[2], (MEMBERS,), ((0, 8),), -0.2, 0.2)), 0.3, 3.0),
        "var_weight": jnp.clip(jnp.exp(jax.random.uniform(keys[3], (VARS,), jnp.float32, math.log(0.3), math.log(3.0))), 0.3, 3.0),
        "embed_in": normal_values(keys[4], (VARS, D), VARS ** -0.5, 0.625),
        "embed_out": normal_values(keys[5], (D, D), D ** -0.5, 0.25),
        "norm_gain": jnp.clip(1.0 + 0.18 * jax.random.normal(keys[6], (D,), jnp.float32), 0.1, 1.9),
        "qkv_weight": normal_values(keys[7], (3, D, D), D ** -0.5, 0.25),
        "head_scale": jnp.clip(jnp.exp(jax.random.uniform(keys[8], (HEADS,), jnp.float32, math.log(1.0), math.log(4.0))), 1.0, 4.0),
        "out_weight": normal_values(keys[9], (D, D), D ** -0.5, 0.25),
        "dec_weight": normal_values(keys[10], (D, VARS), D ** -0.5, 0.25),
        "g2m_node": draw_g2m_node(jax.random.fold_in(keys[14], 71), 0),
        "m2g_node": draw_m2g_node(jax.random.fold_in(keys[14], 71), 0),
        "neighbours": draw_neighbours(jax.random.fold_in(keys[14], 71), 0),
    }


def reference(noisy_state, target_state, noise_level, var_weight, embed_in, embed_out, norm_gain, qkv_weight, head_scale, out_weight, dec_weight, g2m_node, m2g_node, neighbours):
    positions = jnp.arange(GRID).astype(jnp.float32)
    lat_weight = 0.2 + jnp.cos(math.pi * (positions + 0.5) / GRID - 0.5 * math.pi)
    weights_all = var_weight[:, None] * lat_weight[None, :]
    scale_all = 1.0 / (MEMBERS * VARS)
    flat_nbrs = neighbours.reshape(MESH * NBR)

    def by_head(values):
        return values.reshape(MESH, HEADS, HEAD_DIM).transpose(1, 0, 2)

    def unit_rows(values):
        return values * lax.rsqrt(lax.optimization_barrier(jnp.mean(values * values, axis=-1, keepdims=True)) + 1e-06)

    def one_member(inputs):
        state_now, target_now, level = inputs
        level_sq = level * level + 1.0
        scale_in = lax.rsqrt(level_sq)
        skip_scale = 1.0 / level_sq
        out_scale = level * scale_in
        projected = jnp.dot(state_now.T, embed_in, preferred_element_type=jnp.float32)
        hidden = jax.nn.silu(scale_in * projected).astype(jnp.bfloat16)
        encoded = jnp.dot(hidden, embed_out, preferred_element_type=jnp.float32)
        mesh_in = jax.ops.segment_sum(encoded, g2m_node, num_segments=MESH)
        mean_sq = lax.optimization_barrier(jnp.mean(mesh_in * mesh_in, axis=-1, keepdims=True))
        normed = (mesh_in * lax.rsqrt(mean_sq + 1e-05) * norm_gain).astype(jnp.bfloat16)
        queries = jnp.dot(normed, qkv_weight[0], preferred_element_type=jnp.float32)
        key_rows = jnp.dot(normed, qkv_weight[1], preferred_element_type=jnp.float32)
        value_rows = jnp.dot(normed, qkv_weight[2], preferred_element_type=jnp.float32)
        unit_q = by_head(unit_rows(queries.reshape(MESH, HEADS, HEAD_DIM)).astype(jnp.bfloat16).reshape(MESH, D))
        unit_k = by_head(unit_rows(key_rows.reshape(MESH, HEADS, HEAD_DIM)).astype(jnp.bfloat16).reshape(MESH, D))
        value_heads = by_head(value_rows.astype(jnp.bfloat16))

        def attend(parts):
            query_h, key_h, value_h, scale_h = parts
            key_near = key_h[neighbours].astype(jnp.float32)
            scores = jnp.einsum('nd,njd->nj', query_h.astype(jnp.float32), key_near) * scale_h / HEAD_DIM
            exps = jnp.exp(scores)
            attn_probs = (exps / lax.optimization_barrier(jnp.sum(exps, axis=-1, keepdims=True))).astype(jnp.bfloat16)
            mixed_rows = jnp.einsum('nj,njd->nd', attn_probs.astype(jnp.float32), value_h[neighbours].astype(jnp.float32))
            return (mixed_rows.astype(jnp.bfloat16), attn_probs)
        mixed_heads, prob_heads = lax.map(attend, (unit_q, unit_k, value_heads, head_scale))
        attended = mixed_heads.transpose(1, 0, 2).reshape(MESH, D)
        mesh_out = (mesh_in + jnp.dot(attended, out_weight, preferred_element_type=jnp.float32)).astype(jnp.bfloat16)
        decoded = mesh_out[m2g_node]
        net = lax.dot_general(dec_weight, decoded, (((0,), (1,)), ((), ())), preferred_element_type=jnp.float32)
        errors = skip_scale * state_now.astype(jnp.float32) + out_scale * net - target_now.astype(jnp.float32)
        loss_part = jnp.sum(weights_all * errors * errors) * scale_all
        grad_net = (2.0 * out_scale * scale_all * weights_all * errors).astype(jnp.bfloat16)
        grad_dec = lax.dot_general(decoded, grad_net, (((0,), (1,)), ((), ())), preferred_element_type=jnp.float32)
        cell_terms = lax.dot_general(grad_net, dec_weight, (((0,), (1,)), ((), ())), preferred_element_type=jnp.float32)
        mesh_grad = jax.ops.segment_sum(cell_terms, m2g_node, num_segments=MESH).astype(jnp.bfloat16)
        grad_out = lax.dot_general(attended, mesh_grad, (((0,), (0,)), ((), ())), preferred_element_type=jnp.float32)
        head_grad = lax.dot_general(mesh_grad, out_weight, (((1,), (1,)), ((), ())), preferred_element_type=jnp.float32).astype(jnp.bfloat16)

        def spread(parts):
            prob_h, grad_h = parts
            contrib = prob_h.astype(jnp.float32)[:, :, None] * grad_h.astype(jnp.float32)[:, None, :]
            return jax.ops.segment_sum(contrib.reshape(MESH * NBR, HEAD_DIM), flat_nbrs, num_segments=MESH)
        value_grad = lax.map(spread, (prob_heads, by_head(head_grad))).transpose(1, 0, 2).reshape(MESH, D).astype(jnp.bfloat16)
        grad_value = lax.dot_general(normed, value_grad, (((0,), (0,)), ((), ())), preferred_element_type=jnp.float32)
        return (loss_part, grad_dec, grad_out, grad_value)
    totals = lax.map(one_member, (noisy_state, target_state, noise_level))
    return (jnp.sum(totals[0]) / GRID, lax.optimization_barrier(jnp.sum(totals[1], axis=0)), lax.optimization_barrier(jnp.sum(totals[2], axis=0)), lax.optimization_barrier(jnp.sum(totals[3], axis=0)))
```

```python
import math

import jax
import jax.numpy as jnp
from jax import lax
from jax.experimental import pallas as pl
from jax.experimental.pallas import tpu as pltpu
from jax.sharding import PartitionSpec as P

D = 512
VARS = 84
HEADS = 4
G_DEV = 2048
M_DEV = 512
MEM_DEV = 1
HEAD_DIM = 128


MESH_ID = pl.DeviceIdType.MESH
AR_ROWS = (2048, 2048, 512)
AR_AXES = (("x", "y", "z"), ("y", "z", "x"), ("z", "x", "y"))


def coordinates():
    band, chan, core = (lax.axis_index("band"), lax.axis_index("chan"), lax.axis_index("member"))
    return {"band": band, "x": chan, "y": lax.rem(band, 4), "z": band // 4, "core": core}


def peer_on(axis, at, step):
    other = lax.rem(at[axis] + step, 4)
    if axis == "x":
        return (at["band"], other, at["core"])
    if axis == "y":
        return (at["z"] * 4 + other, at["x"], at["core"])
    return (other * 4 + at["y"], at["x"], at["core"])


def sibling(at):
    return (at["band"], at["x"], 1 - at["core"])


class Copies:
    def __init__(self, send_sems, recv_sems):
        self.send_sems, self.recv_sems, self.used = send_sems, recv_sems, 0

    def start(self, source, target, device):
        copy = pltpu.make_async_remote_copy(
            src_ref=source,
            dst_ref=target,
            send_sem=self.send_sems.at[self.used],
            recv_sem=self.recv_sems.at[self.used],
            device_id=device,
            device_id_type=MESH_ID,
        )
        self.used += 1
        copy.start()
        return copy


def sum_scratch():
    shapes = []
    for rows in AR_ROWS:
        half = rows // 2
        shapes += [
            pltpu.VMEM((half, 128), jnp.float32),
            pltpu.VMEM((half, 128), jnp.float32),
            pltpu.VMEM((3, half // 4, 128), jnp.float32),
            pltpu.VMEM((half // 4, 128), jnp.float32),
            pltpu.VMEM((3, half // 16, 128), jnp.float32),
            pltpu.VMEM((4, half // 16, 128), jnp.float32),
            pltpu.VMEM((half // 16, 128), jnp.float32),
        ]
    return shapes


def all_sum(parts, totals, scratch, copies):
    at = coordinates()
    colors = range(len(parts))
    held = [scratch[7 * c : 7 * c + 7] for c in colors]
    half = [rows // 2 for rows in AR_ROWS]
    mine = [pl.multiple_of(at["core"] * half[c], half[c]) for c in colors]
    other = [pl.multiple_of((1 - at["core"]) * half[c], half[c]) for c in colors]
    pending = []
    flights = [
        copies.start(parts[c].at[pl.ds(other[c], half[c]), :], held[c][0], sibling(at)) for c in colors
    ]
    for c in colors:
        flights[c].wait_recv()
        held[c][1][...] = parts[c][pl.ds(mine[c], half[c]), :] + held[c][0][...]
    pending += flights

    def scatter(source, landing, size, axis, c):
        sent = []
        for step in (1, 2, 3):
            slot = lax.rem(at[axis] + step, 4)
            rows = pl.ds(pl.multiple_of(slot * size, size), size)
            sent.append(copies.start(source.at[rows, :], landing.at[step - 1], peer_on(axis, at, step)))
        return sent

    def gather_sum(source, landing, result, size, axis, sent):
        for flight in sent:
            flight.wait_recv()
        rows = pl.ds(pl.multiple_of(at[axis] * size, size), size)
        result[...] = (source[rows, :] + landing[0]) + (landing[1] + landing[2])

    def spread(c, start, size, axis):
        rows = totals[c].at[pl.ds(pl.multiple_of(start, size), size), :]
        return [copies.start(rows, rows, peer_on(axis, at, step)) for step in (1, 2, 3)]

    quarter = [h // 4 for h in half]
    tiny = [h // 16 for h in half]
    flights = [scatter(held[c][1], held[c][2], quarter[c], AR_AXES[c][0], c) for c in colors]
    second = []
    for c in colors:
        gather_sum(held[c][1], held[c][2], held[c][3], quarter[c], AR_AXES[c][0], flights[c])
        second.append(scatter(held[c][3], held[c][4], tiny[c], AR_AXES[c][1], c))
        pending += flights[c]
    third = []
    for c in colors:
        gather_sum(held[c][3], held[c][4], held[c][6], tiny[c], AR_AXES[c][1], second[c])
        pending += second[c]
        axis = AR_AXES[c][2]
        held[c][5][at[axis]] = held[c][6][...]
        third.append(
            [copies.start(held[c][6], held[c][5].at[at[axis]], peer_on(axis, at, step)) for step in (1, 2, 3)]
        )
    fourth = []
    first = [mine[c] + at[AR_AXES[c][0]] * quarter[c] for c in colors]
    inner = [first[c] + at[AR_AXES[c][1]] * tiny[c] for c in colors]
    for c in colors:
        for flight in third[c]:
            flight.wait_recv()
        pending += third[c]
        slots = held[c][5]
        totals[c][pl.ds(pl.multiple_of(inner[c], tiny[c]), tiny[c]), :] = (slots[0] + slots[1]) + (
            slots[2] + slots[3]
        )
        fourth.append(spread(c, inner[c], tiny[c], AR_AXES[c][1]))
    fifth = []
    for c in colors:
        for flight in fourth[c]:
            flight.wait_recv()
        pending += fourth[c]
        fifth.append(spread(c, first[c], quarter[c], AR_AXES[c][0]))
    last = []
    for c in colors:
        for flight in fifth[c]:
            flight.wait_recv()
        pending += fifth[c]
        rows = totals[c].at[pl.ds(mine[c], half[c]), :]
        last.append(copies.start(rows, rows, sibling(at)))
    for c in colors:
        last[c].wait_recv()
    pending += last
    for flight in pending:
        flight.wait_send()


def greet(devices):
    barrier = pltpu.get_barrier_semaphore()
    for device in devices:
        pl.semaphore_signal(barrier, inc=1, device_id=device, device_id_type=MESH_ID)
    pl.semaphore_wait(barrier, len(devices))


def sum_partners(at):
    return [sibling(at)] + [peer_on(axis, at, step) for axis in ("x", "y", "z") for step in (1, 2, 3)]


def sum_kernel(out_ref, value_ref, dec_ref, out_total, value_total, dec_total, *scratch):
    parts, totals, rest = scratch[:2], scratch[2:4], scratch[4:]
    held, (send_sems, recv_sems) = rest[:-2], rest[-2:]
    for source, part in ((out_ref, parts[0]), (value_ref, parts[1])):
        for lane in range(4):
            part[512 * lane : 512 * lane + 512, :] = source[:, 128 * lane : 128 * lane + 128]
    greet(sum_partners(coordinates()))
    all_sum((*parts, dec_ref), (*totals, dec_total), held, Copies(send_sems, recv_sems))
    for total, result in zip(totals, (out_total, value_total)):
        for lane in range(4):
            result[:, 128 * lane : 128 * lane + 128] = total[512 * lane : 512 * lane + 512, :]


def device_sum(loss_part, grad_dec, grad_out, grad_value):
    dec = jnp.pad(grad_dec, ((0, 0), (0, 128 - VARS))).at[0, 127].set(loss_part)
    square = jax.ShapeDtypeStruct((D, D), jnp.float32)
    vmem = pl.BlockSpec(memory_space=pltpu.VMEM)
    totals = pl.pallas_call(
        sum_kernel,
        out_shape=(square, square, jax.ShapeDtypeStruct((D, 128), jnp.float32)),
        in_specs=[vmem] * 3,
        out_specs=(vmem,) * 3,
        scratch_shapes=[pltpu.VMEM((2048, 128), jnp.float32)] * 4
        + sum_scratch()
        + [pltpu.SemaphoreType.DMA((64,)), pltpu.SemaphoreType.DMA((64,))],
        compiler_params=pltpu.CompilerParams(collective_id=0, has_side_effects=True),
        name="device_sum",
    )(grad_out, grad_value, dec)
    return totals[2][0, 127], totals[2][:, :VARS], totals[0], totals[1]


def with_halo(array, sides, width):
    for axis, dim in sides:
        size, length = (lax.axis_size(axis), array.shape[dim])
        up = [(i, (i + 1) % size) for i in range(size - 1)]
        down = [(j, i) for i, j in up]
        last = lax.slice_in_dim(array, length - width, length, axis=dim)
        leading = lax.slice_in_dim(array, 0, width, axis=dim)
        before = lax.ppermute(last, axis, up)
        after = lax.ppermute(leading, axis, down)
        array = jnp.concatenate([before, array, after], axis=dim)
    return array


def rim_parts(partial_value, rows_patch):
    return jnp.concatenate([partial_value[:rows_patch], partial_value[2 * rows_patch :]], axis=0)


def with_rims(partial_value, grown, rows_patch):
    return partial_value[rows_patch : 2 * rows_patch] + grown[:rows_patch] + grown[3 * rows_patch :]


def unit_rows(values):
    return values * lax.rsqrt(jnp.mean(values * values, axis=-1, keepdims=True) + 1e-06)


def split_parts(values, count):
    pieces = []
    rest = values
    for index in range(count):
        piece = lax.optimization_barrier(rest.astype(jnp.bfloat16))
        pieces.append(piece)
        rest = rest - piece.astype(jnp.float32)
    return pieces


def split_einsum(form, left, right_values, count):
    total = None
    for piece in split_parts(right_values, count):
        term = jnp.einsum(form, left, piece, preferred_element_type=jnp.float32)
        total = term if total is None else total + term
    return total


def local(
    noisy_state,
    target_state,
    noise_level,
    var_weight,
    embed_in,
    embed_out,
    norm_gain,
    qkv_weight,
    head_scale,
    out_weight,
    dec_weight,
    g2m_node,
    m2g_node,
    neighbours,
):
    band_index = lax.axis_index("band")
    band_count = lax.axis_size("band")
    members_all = MEM_DEV * lax.axis_size("chan") * lax.axis_size("member")
    base_node = (band_index - 1) * M_DEV
    scale_all = 1.0 / (members_all * VARS)
    level_sq = noise_level * noise_level + 1.0
    scale_in = lax.rsqrt(level_sq)
    skip_scale = 1.0 / level_sq
    out_scale = noise_level * scale_in
    node_ids = jnp.arange(3 * M_DEV, dtype=jnp.int32)
    projected = jnp.einsum("mvg,vd->gmd", noisy_state, embed_in, preferred_element_type=jnp.float32)
    hidden = jax.nn.silu(scale_in[None, :, None] * projected).astype(jnp.bfloat16)
    enc_table = ((g2m_node - base_node)[:, None] == node_ids[None, :]).astype(jnp.bfloat16)
    node_hidden = jnp.einsum("gp,gmd->pmd", enc_table, hidden, preferred_element_type=jnp.float32)
    enc_part = split_einsum("de,pmd->pme", embed_out, node_hidden, 3)
    enc_grown = with_halo(rim_parts(enc_part, M_DEV), (("band", 0),), M_DEV)
    mesh_in = with_rims(enc_part, enc_grown, M_DEV)
    mean_sq = jnp.mean(mesh_in * mesh_in, axis=-1, keepdims=True)
    normed = (mesh_in * lax.rsqrt(mean_sq + 1e-05) * norm_gain).astype(jnp.bfloat16)
    queries = unit_rows(
        jnp.einsum(
            "nmd,de->nme", normed, qkv_weight[0], preferred_element_type=jnp.float32
        ).reshape(M_DEV, MEM_DEV, HEADS, HEAD_DIM)
    ).astype(jnp.bfloat16)
    wider = with_halo(normed, (("band", 0),), M_DEV)
    pair = jnp.einsum(
        "nmd,tde->tnme", wider, qkv_weight[1:], preferred_element_type=jnp.float32
    ).reshape(2, 3 * M_DEV, MEM_DEV, HEADS, HEAD_DIM)
    nearby = jnp.stack([unit_rows(pair[0]).astype(jnp.bfloat16), pair[1].astype(jnp.bfloat16)])
    local_nbrs = neighbours - base_node
    block_rows = math.gcd(M_DEV, max(8, 512 // MEM_DEV))
    block_count = M_DEV // block_rows

    def block_weights():
        scores = (
            jnp.einsum("nmhe,pmhe->nmhp", queries, nearby[0], preferred_element_type=jnp.float32)
            * (head_scale / HEAD_DIM)[None, None, :, None]
        )
        counts = jnp.sum(
            (local_nbrs[:, :, None] == node_ids[None, None, :]).astype(jnp.float32), axis=1
        )[:, None, None, :]
        exps = jnp.exp(scores)
        attn_probs = (exps / jnp.sum(counts * exps, axis=-1, keepdims=True)).astype(jnp.bfloat16)
        return counts * attn_probs.astype(jnp.float32)

    def attend(block_index):
        weights = block_weights()
        mixed_rows = None
        for piece in split_parts(weights, 2):
            term = jnp.einsum(
                "nmhp,pmhe->nmhe", piece, nearby[1], preferred_element_type=jnp.float32
            )
            mixed_rows = term if mixed_rows is None else mixed_rows + term
        return mixed_rows.astype(jnp.bfloat16)

    mixed_blocks = lax.map(attend, jnp.arange(block_count))
    attended = mixed_blocks.reshape(M_DEV, MEM_DEV, D)
    mesh_out = (
        mesh_in
        + jnp.einsum("nmd,de->nme", attended, out_weight, preferred_element_type=jnp.float32)
    ).astype(jnp.bfloat16)
    dec_table = ((m2g_node - base_node)[:, None] == node_ids[None, :]).astype(jnp.bfloat16)
    node_vars = jnp.einsum("nmc,cv->nmv", mesh_out, dec_weight, preferred_element_type=jnp.float32)
    vars_wide = with_halo(node_vars, (("band", 0),), M_DEV)
    net_full = split_einsum("gp,pmv->mvg", dec_table, vars_wide, 3)
    positions = (band_index * G_DEV + jnp.arange(G_DEV)).astype(jnp.float32)
    lat_weight = 0.2 + jnp.cos(math.pi * (positions + 0.5) / (G_DEV * band_count) - 0.5 * math.pi)
    weights_all = var_weight[:, None] * lat_weight[None, :]
    errors = (
        skip_scale[:, None, None] * noisy_state.astype(jnp.float32)
        + out_scale[:, None, None] * net_full
        - target_state.astype(jnp.float32)
    )
    loss_part = jnp.sum(weights_all * errors * errors) * scale_all
    grad_net = ((2.0 * out_scale * scale_all)[:, None, None] * weights_all * errors).astype(
        jnp.bfloat16
    )
    node_part = jnp.einsum("gp,mvg->pmv", dec_table, grad_net, preferred_element_type=jnp.float32)
    node_grown = with_halo(
        rim_parts(node_part, M_DEV).astype(jnp.bfloat16), (("band", 0),), M_DEV
    ).astype(jnp.float32)
    node_grad = with_rims(node_part, node_grown, M_DEV)
    grad_dec = jnp.einsum(
        "nmc,nmv->cv", mesh_out.astype(jnp.float32), node_grad, precision=lax.Precision.HIGHEST
    )
    mesh_grad = jnp.einsum(
        "nmv,cv->nmc", node_grad, dec_weight.astype(jnp.float32), precision=lax.Precision.HIGHEST
    ).astype(jnp.bfloat16)
    grad_out = jnp.einsum("nmd,nmc->dc", attended, mesh_grad, preferred_element_type=jnp.float32)
    head_grad = jnp.einsum(
        "nmc,dc->nmd", mesh_grad, out_weight, preferred_element_type=jnp.float32
    ).astype(jnp.bfloat16)
    head_grad = head_grad.reshape(M_DEV, MEM_DEV, HEADS, HEAD_DIM)

    def spread(carry, block_index):
        weights = block_weights()
        for piece in split_parts(weights, 2):
            carry = carry + jnp.einsum(
                "nmhp,nmhe->pmhe", piece, head_grad, preferred_element_type=jnp.float32
            )
        return (carry, None)

    empty_sums = jnp.zeros((3 * M_DEV, MEM_DEV, HEADS, HEAD_DIM), jnp.float32)
    value_part, unused_out = lax.scan(spread, empty_sums, jnp.arange(block_count))
    value_part = value_part.reshape(3 * M_DEV, MEM_DEV, D)
    value_grown = with_halo(
        rim_parts(value_part, M_DEV).astype(jnp.bfloat16), (("band", 0),), M_DEV
    ).astype(jnp.float32)
    value_grad = with_rims(value_part, value_grown, M_DEV).astype(jnp.bfloat16)
    grad_value = jnp.einsum("nmd,nmc->dc", normed, value_grad, preferred_element_type=jnp.float32)
    totals = device_sum(loss_part, grad_dec, grad_out, grad_value)
    loss_value = totals[0] / (G_DEV * band_count)
    return (loss_value, totals[1], totals[2], totals[3])


def solution(mesh):
    in_specs = (
        P(("chan", "member"), None, "band"),
        P(("chan", "member"), None, "band"),
        P(("chan", "member")),
        P(),
        P(),
        P(),
        P(),
        P(),
        P(),
        P(),
        P(),
        P("band"),
        P("band"),
        P("band", None),
    )
    out_specs = (P(), P(), P(), P())
    return jax.shard_map(local, mesh=mesh, in_specs=in_specs, out_specs=out_specs, check_vma=False)
```

```python
import math

import jax
import jax.numpy as jnp
from jax import lax
from jax.experimental import pallas as pl
from jax.experimental.pallas import tpu as pltpu
from jax.sharding import PartitionSpec as P

D = 512
VARS = 84
HEADS = 4
NBR = 32
G_DEV = 2048
M_DEV = 512
HEAD_DIM = 128
GRID = 32768
MEMBERS = 8
WINDOW = 3 * M_DEV
ROWS = 96
BF16, F32, I32 = jnp.bfloat16, jnp.float32, jnp.int32
MESH_ID = pl.DeviceIdType.MESH
SUM_ROWS = {"out": 2048, "value": 2048, "dec": 512}
SUM_AXES = {"out": ("x", "y", "z"), "value": ("y", "z", "x"), "dec": ("z", "x", "y")}


def coordinates():
    band, chan, core = (lax.axis_index("band"), lax.axis_index("chan"), lax.axis_index("member"))
    return {"band": band, "x": chan, "y": lax.rem(band, 4), "z": band // 4, "core": core}


def peer_on(axis, at, step):
    other = lax.rem(at[axis] + step, 4)
    if axis == "x":
        return (at["band"], other, at["core"])
    if axis == "y":
        return (at["z"] * 4 + other, at["x"], at["core"])
    return (other * 4 + at["y"], at["x"], at["core"])


def sibling(at):
    return (at["band"], at["x"], 1 - at["core"])


class Copies:
    def __init__(self, send_sems, recv_sems):
        self.send_sems, self.recv_sems, self.all = send_sems, recv_sems, []

    def start(self, source, target, device):
        used = len(self.all)
        copy = pltpu.make_async_remote_copy(
            src_ref=source,
            dst_ref=target,
            send_sem=self.send_sems.at[used],
            recv_sem=self.recv_sems.at[used],
            device_id=device,
            device_id_type=MESH_ID,
        )
        self.all.append(copy)
        copy.start()
        return copy


def greet(devices):
    barrier = pltpu.get_barrier_semaphore()
    for device in devices:
        pl.semaphore_signal(barrier, inc=1, device_id=device, device_id_type=MESH_ID)
    pl.semaphore_wait(barrier, len(devices))


def sum_partners(at):
    return [sibling(at)] + [peer_on(axis, at, step) for axis in ("x", "y", "z") for step in (1, 2, 3)]


def sum_scratch(rows):
    half = rows // 2
    return [
        pltpu.VMEM((rows, 128), F32),
        pltpu.VMEM((rows, 128), F32),
        pltpu.VMEM((half, 128), F32),
        pltpu.VMEM((half, 128), F32),
        pltpu.VMEM((3, half // 4, 128), F32),
        pltpu.VMEM((half // 4, 128), F32),
        pltpu.VMEM((3, half // 16, 128), F32),
        pltpu.VMEM((4, half // 16, 128), F32),
        pltpu.VMEM((half // 16, 128), F32),
    ]


def device_sum(name, refs, copies, at):
    part, total, near, pair, first_in, first, second_in, slots, second = refs
    first_axis, second_axis, third_axis = SUM_AXES[name]
    half = SUM_ROWS[name] // 2
    quarter, tiny = half // 4, half // 16

    def rows(start, size):
        return pl.ds(pl.multiple_of(start, size), size)

    def scatter(source, landing, size, axis):
        sent = []
        for step in (1, 2, 3):
            block = source.at[rows(lax.rem(at[axis] + step, 4) * size, size), :]
            sent.append(copies.start(block, landing.at[step - 1], peer_on(axis, at, step)))
        return sent

    def gather_sum(source, landing, size, axis, sent):
        for flight in sent:
            flight.wait_recv()
        return (source[rows(at[axis] * size, size), :] + landing[0]) + (landing[1] + landing[2])

    def spread(start, size, axis):
        block = total.at[rows(start, size), :]
        return [copies.start(block, block, peer_on(axis, at, step)) for step in (1, 2, 3)]

    mine = at["core"] * half
    flight = copies.start(part.at[rows((1 - at["core"]) * half, half), :], near, sibling(at))
    yield
    flight.wait_recv()
    pair[...] = part[rows(mine, half), :] + near[...]
    flights = scatter(pair, first_in, quarter, first_axis)
    yield
    first[...] = gather_sum(pair, first_in, quarter, first_axis, flights)
    flights = scatter(first, second_in, tiny, second_axis)
    yield
    second[...] = gather_sum(first, second_in, tiny, second_axis, flights)
    slots[at[third_axis]] = second[...]
    flights = [
        copies.start(second, slots.at[at[third_axis]], peer_on(third_axis, at, step)) for step in (1, 2, 3)
    ]
    yield
    for flight in flights:
        flight.wait_recv()
    outer = mine + at[first_axis] * quarter
    inner = outer + at[second_axis] * tiny
    total[rows(inner, tiny), :] = (slots[0] + slots[1]) + (slots[2] + slots[3])
    flights = spread(inner, tiny, second_axis)
    yield
    for flight in flights:
        flight.wait_recv()
    flights = spread(outer, quarter, first_axis)
    yield
    for flight in flights:
        flight.wait_recv()
    block = total.at[rows(mine, half), :]
    flight = copies.start(block, block, sibling(at))
    yield
    flight.wait_recv()
    yield


def dot(left, right):
    return jnp.dot(left, right, preferred_element_type=F32)


def dot_t(left, right):
    return lax.dot_general(left, right, (((1,), (1,)), ((), ())), preferred_element_type=F32)


def pieces_of(values, count):
    pieces, rest = ([], values)
    for index in range(count):
        piece = rest.astype(BF16)
        pieces.append(piece)
        if index + 1 < count:
            rest = rest - piece.astype(F32)
    return pieces


def column_of(row, size):
    tall = jnp.transpose(jnp.broadcast_to(row, (128, size)))
    return tall


def unit_heads(values, width):
    split = values.reshape(HEADS, HEAD_DIM, width)
    scale = lax.rsqrt(jnp.mean(split * split, axis=1, keepdims=True) + 1e-06)
    return (split * scale).reshape(D, width)


def lanes(values, width):
    return jnp.concatenate([values] * (width // 128), axis=1)


def step_kernel(
    noisy_ref,
    target_ref,
    level_ref,
    var_ref,
    embed_in_ref,
    embed_out_ref,
    gain_ref,
    qkv_ref,
    head_scale_ref,
    out_w_ref,
    dec_w_ref,
    g2m_ref,
    m2g_ref,
    nbr_ref,
    lat_ref,
    out_result,
    value_result,
    dec_result,
    *scratch,
):
    send_sems, recv_sems = scratch[:2]
    (
        state_in,
        g2m_in,
        pad_in,
        pad_dec,
        embed_in_t,
        embed_out_t,
        q_t,
        k_t,
        v_t,
        out_t,
        dec_t,
        node_hidden,
        mesh_in,
        normed,
        normed_in,
        unit_q,
        unit_k,
        values,
        counts,
        counts_16,
        exps,
        probs,
        attended,
        mesh_out,
        table,
        vars_own,
        vars_16,
        vars_in,
        net,
        grad_net,
        node_out,
        node_in,
        node_own,
        mesh_grad,
        head_grad,
        value_out,
        value_in,
        value_own,
    ) = scratch[2:40]
    sums = {name: scratch[40 + 9 * i : 49 + 9 * i] for i, name in enumerate(("out", "value", "dec"))}
    at = coordinates()
    band = at["band"]
    left = (lax.rem(band + 15, 16), at["x"], at["core"])
    right = (lax.rem(band + 1, 16), at["x"], at["core"])
    sides = ((0, left, 1), (1, right, 0))
    base = band * M_DEV
    copies = Copies(send_sems, recv_sems)

    greet([left, right] + sum_partners(at))

    state_flights, node_flights = ([], [])
    for side, device, slot in sides:
        node_flights.append(copies.start(g2m_ref, g2m_in.at[slot], device))
    for chunk in range(4):
        cells = pl.ds(512 * chunk, 512)
        state_flights.append(
            [
                copies.start(noisy_ref.at[0, :, cells], state_in.at[slot, :, cells], device)
                for side, device, slot in sides
            ]
        )

    pad_in[...] = jnp.zeros_like(pad_in)
    pad_dec[...] = jnp.zeros_like(pad_dec)
    pad_in[:VARS, :] = embed_in_ref[...]
    pad_dec[:, :VARS] = dec_w_ref[...]
    embed_in_t[...] = jnp.transpose(pad_in[...])
    dec_t[...] = jnp.transpose(pad_dec[...])
    embed_out_t[...] = jnp.transpose(embed_out_ref[...])
    q_t[...] = jnp.transpose(qkv_ref[0])
    k_t[...] = jnp.transpose(qkv_ref[1])
    v_t[...] = jnp.transpose(qkv_ref[2])
    out_t[...] = jnp.transpose(out_w_ref[...])

    level = jnp.full((1, 1), level_ref[0], F32)
    level_sq = level * level + 1.0
    scale_in = lax.rsqrt(level_sq)
    skip_scale = 1.0 / level_sq
    out_scale = level * scale_in
    half_scale = 0.5 * scale_in

    def encode(state, nodes):
        half_t = dot(embed_in_t[:, :VARS], state) * half_scale
        hidden = (half_t + half_t * jnp.tanh(half_t)).astype(BF16)
        ids = lax.broadcasted_iota(I32, (M_DEV, 512), 0)
        chosen = jnp.where(nodes - base == ids, 1.0, 0.0).astype(BF16)
        node_hidden[...] += dot_t(hidden, chosen)

    node_hidden[...] = jnp.zeros_like(node_hidden)

    @pl.loop(0, 4)
    def _(chunk):
        cells = pl.ds(pl.multiple_of(chunk * 512, 512), 512)
        encode(noisy_ref[0, :, cells], g2m_ref[:, cells])

    @pl.loop(0, 8)
    def _(block):
        ids = lax.broadcasted_iota(I32, (64, M_DEV), 0) + block * 64
        total = jnp.zeros((64, M_DEV), I32)
        for j in range(NBR):
            near = nbr_ref[j : j + 1, :] - (base - M_DEV)
            patch = near // M_DEV
            within = near - patch * M_DEV
            field = jnp.where(patch == 0, 64, jnp.where(patch == 1, 1, 4096))
            total = total + jnp.where(within == ids, field, 0)
        chunk = block // 2
        part = (block - 2 * chunk) * 64
        for start, shift in (
            (block * 64, 0),
            (M_DEV + 256 * chunk + part, 6),
            (M_DEV + 256 * chunk + 128 + part, 12),
        ):
            count = lax.shift_right_logical(total, jnp.full_like(total, shift)) & 63
            rows = pl.ds(pl.multiple_of(start, 64), 64)
            counts[rows, :] = count.astype(F32)
            counts_16[rows, :] = count.astype(F32).astype(BF16)

    for block in range(12):
        if block < 4:
            offset = 128 * block
        else:
            offset = 128 * ((block - 4) // 2) + (M_DEV if (block - 4) % 2 else -M_DEV)
        ids = lax.broadcasted_iota(I32, (128, G_DEV), 0) + (base + offset)
        table[128 * block : 128 * block + 128, :] = jnp.where(m2g_ref[...] == ids, 1.0, 0.0).astype(BF16)

    for flight in node_flights:
        flight.wait_recv()
    for chunk in range(4):
        cells = slice(512 * chunk, 512 * chunk + 512)
        for flight in state_flights[chunk]:
            flight.wait_recv()

        @pl.loop(0, 2)
        def _(slot):
            encode(state_in[slot, :, cells], g2m_in[slot, :, cells])

    encoded = None
    for piece in pieces_of(node_hidden[...], 3):
        term = dot(embed_out_t[...], piece)
        encoded = term if encoded is None else encoded + term
    mesh_in[...] = encoded
    mean_sq = jnp.mean(encoded * encoded, axis=0, keepdims=True)
    gain = lanes(column_of(gain_ref[...], D), M_DEV)
    normed[...] = (encoded * lax.rsqrt(mean_sq + 1e-05) * gain).astype(BF16)

    normed_flights = []
    for chunk in range(4):
        normed_flights.append(
            [
                copies.start(
                    normed.at[:, pl.ds(128 * chunk, 128)],
                    normed_in.at[:, pl.ds(256 * chunk + 128 * slot, 128)],
                    device,
                )
                for side, device, slot in sides
            ]
        )

    unit_q[...] = unit_heads(dot(q_t[...], normed[...]), M_DEV).astype(BF16)

    def attend(near, start, width):
        keys = unit_heads(dot(k_t[...], near), width).astype(BF16)
        unit_k[start : start + width, :] = jnp.transpose(keys)
        values[:, start : start + width] = dot(v_t[...], near).astype(BF16)
        sums_now = []
        count = counts[start : start + width, :]
        for head in range(HEADS):
            part = slice(HEAD_DIM * head, HEAD_DIM * head + HEAD_DIM)
            scores = dot(unit_k[start : start + width, part], unit_q[part, :])
            exp = jnp.exp(scores * (head_scale_ref[head] / HEAD_DIM))
            exps[head, start : start + width, :] = exp
            sums_now.append(jnp.sum(exp * count, axis=0, keepdims=True))
        return sums_now

    exp_sums = None
    for chunk in range(6):
        if chunk < 2:
            near = normed[:, 256 * chunk : 256 * chunk + 256]
        else:
            for flight in normed_flights[chunk - 2]:
                flight.wait_recv()
            near = normed_in[:, 256 * (chunk - 2) : 256 * (chunk - 2) + 256]
        sums_now = attend(near, 256 * chunk, 256)
        exp_sums = sums_now if exp_sums is None else [a + b for a, b in zip(exp_sums, sums_now)]

    for head in range(HEADS):
        inverse = 1.0 / exp_sums[head]
        part = slice(HEAD_DIM * head, HEAD_DIM * head + HEAD_DIM)

        @pl.loop(0, 6)
        def _(block):
            rows = pl.ds(pl.multiple_of(block * 256, 256), 256)
            prob = (exps[head, rows, :] * inverse).astype(BF16)
            probs[head, rows, :] = prob * counts_16[rows, :]

        attended[part, :] = dot(values[part, :], probs[head]).astype(BF16)

    mesh_out[...] = (mesh_in[...] + dot(out_t[...], attended[...])).astype(BF16)
    vars_own[...] = dot(dec_t[:ROWS, :], mesh_out[...])

    vars_flights = []
    for chunk in range(4):
        vars_flights.append(
            [
                copies.start(
                    vars_own.at[:, pl.ds(128 * chunk, 128)],
                    vars_in.at[:, pl.ds(256 * chunk + 128 * slot, 128)],
                    device,
                )
                for side, device, slot in sides
            ]
        )

    def split_rows(source):
        for index, piece in enumerate(pieces_of(source, 2)):
            vars_16[ROWS * index : ROWS * index + ROWS, : source.shape[1]] = piece

    def decode(width, start, first):
        @pl.loop(0, 4)
        def _(chunk):
            cells = pl.ds(pl.multiple_of(chunk * 512, 512), 512)
            both = dot(vars_16[:, :width], table[start : start + width, cells])
            term = both[:ROWS, :] + both[ROWS:, :]
            net[:, cells] = term if first else net[:, cells] + term

    split_rows(vars_own[...])
    decode(M_DEV, 0, True)
    for pair in vars_flights:
        for flight in pair:
            flight.wait_recv()
    split_rows(vars_in[...])
    decode(2 * M_DEV, M_DEV, False)

    square = lax.broadcasted_iota(I32, (VARS, VARS), 0) == lax.broadcasted_iota(I32, (VARS, VARS), 1)
    var_column = jnp.sum(jnp.where(square, var_ref[...], 0.0), axis=1, keepdims=True)
    weights = var_column * lat_ref[...]
    errors = (
        skip_scale * noisy_ref[0].astype(F32) + out_scale * net[:VARS, :] - target_ref[0].astype(F32)
    )
    scale_all = 1.0 / (MEMBERS * VARS)
    loss = jnp.sum(jnp.sum(weights * errors * errors, axis=1, keepdims=True), axis=0, keepdims=True) * scale_all
    grad_net[...] = jnp.zeros_like(grad_net)
    grad_net[:VARS, :] = ((2.0 * out_scale * scale_all) * weights * errors).astype(BF16)

    node_part = dot_t(grad_net[...], table[M_DEV:, :])
    for chunk in range(4):
        for side in (0, 1):
            start = 256 * chunk + 128 * side
            node_out[side, :, 128 * chunk : 128 * chunk + 128] = node_part[:, start : start + 128].astype(BF16)
    node_flights = [
        copies.start(node_out.at[side], node_in.at[slot], device) for side, device, slot in sides
    ]
    node_own[...] = dot_t(grad_net[...], table[:M_DEV, :])
    for flight in node_flights:
        flight.wait_recv()
    node_grad = node_own[...] + node_in[0].astype(F32) + node_in[1].astype(F32)
    node_pieces = pieces_of(node_grad, 3)
    grown = None
    for piece in node_pieces:
        term = dot(dec_w_ref[...], piece[:VARS, :])
        grown = term if grown is None else grown + term
    mesh_grad[...] = grown.astype(BF16)
    head_grad[...] = dot(out_w_ref[...], mesh_grad[...]).astype(BF16)

    value_flights = []
    for head in range(HEADS):
        part = slice(HEAD_DIM * head, HEAD_DIM * head + HEAD_DIM)
        spread = dot_t(head_grad[part, :], probs[head, M_DEV:, :])
        for chunk in range(4):
            for side in (0, 1):
                start = 256 * chunk + 128 * side
                value_out[side, part, 128 * chunk : 128 * chunk + 128] = spread[
                    :, start : start + 128
                ].astype(BF16)
        rows = pl.ds(HEAD_DIM * head, HEAD_DIM)
        value_flights.append(
            [
                copies.start(value_out.at[side, rows, :], value_in.at[slot, rows, :], device)
                for side, device, slot in sides
            ]
        )

    def store_square(target, source):
        for lane in range(4):
            target[512 * lane : 512 * lane + 512, :] = source[:, 128 * lane : 128 * lane + 128]

    store_square(sums["out"][0], dot_t(attended[...], mesh_grad[...]))
    dec_sum = None
    for piece in node_pieces:
        term = dot_t(mesh_out[...], piece)
        dec_sum = term if dec_sum is None else dec_sum + term
    sums["dec"][0][...] = jnp.zeros_like(sums["dec"][0])
    sums["dec"][0][:, :ROWS] = dec_sum
    corner = (lax.broadcasted_iota(I32, (8, 128), 0) == 0) & (lax.broadcasted_iota(I32, (8, 128), 1) == 127)
    sums["dec"][0][:8, :] = jnp.where(corner, loss, sums["dec"][0][:8, :])
    out_sum = device_sum("out", sums["out"], copies, at)
    dec_sum = device_sum("dec", sums["dec"], copies, at)
    next(out_sum)
    next(dec_sum)
    for head in range(HEADS):
        part = slice(HEAD_DIM * head, HEAD_DIM * head + HEAD_DIM)
        value_own[part, :] = dot_t(head_grad[part, :], probs[head, :M_DEV, :])
    next(out_sum)
    next(dec_sum)
    for head in range(HEADS):
        part = slice(HEAD_DIM * head, HEAD_DIM * head + HEAD_DIM)
        for flight in value_flights[head]:
            flight.wait_recv()
        grad = value_own[part, :] + value_in[0, part, :].astype(F32) + value_in[1, part, :].astype(F32)
        sums["value"][0][512 * head : 512 * head + 512, :] = dot_t(normed[...], grad.astype(BF16))
    value_sum = device_sum("value", sums["value"], copies, at)
    next(value_sum)
    for stage in range(6):
        next(value_sum)
        if stage < 5:
            next(out_sum)
            next(dec_sum)
        if stage == 5:
            next(value_sum)
    next(out_sum)
    next(dec_sum)
    for lane in range(4):
        for name, result in (("out", out_result), ("value", value_result)):
            result[:, 128 * lane : 128 * lane + 128] = sums[name][1][512 * lane : 512 * lane + 512, :]
    dec_result[...] = sums["dec"][1][...]
    for copy in copies.all:
        copy.wait_send()


def local(
    noisy_state,
    target_state,
    noise_level,
    var_weight,
    embed_in,
    embed_out,
    norm_gain,
    qkv_weight,
    head_scale,
    out_weight,
    dec_weight,
    g2m_node,
    m2g_node,
    neighbours,
):
    band = lax.axis_index("band")
    positions = (band * G_DEV + jnp.arange(G_DEV)).astype(F32)
    lat_weight = 0.2 + jnp.cos(math.pi * (positions + 0.5) / GRID - 0.5 * math.pi)
    vmem = pl.BlockSpec(memory_space=pltpu.VMEM)
    smem = pl.BlockSpec(memory_space=pltpu.SMEM)
    square = jax.ShapeDtypeStruct((D, D), F32)
    scratch = [
        pltpu.SemaphoreType.DMA((96,)),
        pltpu.SemaphoreType.DMA((96,)),
        pltpu.VMEM((2, VARS, G_DEV), BF16),
        pltpu.VMEM((2, 1, G_DEV), I32),
        pltpu.VMEM((128, D), BF16),
        pltpu.VMEM((D, 128), BF16),
        pltpu.VMEM((D, 128), BF16),
        pltpu.VMEM((D, D), BF16),
        pltpu.VMEM((D, D), BF16),
        pltpu.VMEM((D, D), BF16),
        pltpu.VMEM((D, D), BF16),
        pltpu.VMEM((D, D), BF16),
        pltpu.VMEM((128, D), BF16),
        pltpu.VMEM((D, M_DEV), F32),
        pltpu.VMEM((D, M_DEV), F32),
        pltpu.VMEM((D, M_DEV), BF16),
        pltpu.VMEM((D, 2 * M_DEV), BF16),
        pltpu.VMEM((D, M_DEV), BF16),
        pltpu.VMEM((WINDOW, D), BF16),
        pltpu.VMEM((D, WINDOW), BF16),
        pltpu.VMEM((WINDOW, M_DEV), F32),
        pltpu.VMEM((WINDOW, M_DEV), BF16),
        pltpu.VMEM((HEADS, WINDOW, M_DEV), F32),
        pltpu.VMEM((HEADS, WINDOW, M_DEV), BF16),
        pltpu.VMEM((D, M_DEV), BF16),
        pltpu.VMEM((D, M_DEV), BF16),
        pltpu.VMEM((WINDOW, G_DEV), BF16),
        pltpu.VMEM((ROWS, M_DEV), F32),
        pltpu.VMEM((2 * ROWS, 2 * M_DEV), BF16),
        pltpu.VMEM((ROWS, 2 * M_DEV), F32),
        pltpu.VMEM((ROWS, G_DEV), F32),
        pltpu.VMEM((ROWS, G_DEV), BF16),
        pltpu.VMEM((2, ROWS, M_DEV), BF16),
        pltpu.VMEM((2, ROWS, M_DEV), BF16),
        pltpu.VMEM((ROWS, M_DEV), F32),
        pltpu.VMEM((D, M_DEV), BF16),
        pltpu.VMEM((D, M_DEV), BF16),
        pltpu.VMEM((2, D, M_DEV), BF16),
        pltpu.VMEM((2, D, M_DEV), BF16),
        pltpu.VMEM((D, M_DEV), F32),
    ]
    for name in ("out", "value", "dec"):
        scratch += sum_scratch(SUM_ROWS[name])
    grad_out, grad_value, dec = pl.pallas_call(
        step_kernel,
        out_shape=(square, square, jax.ShapeDtypeStruct((D, 128), F32)),
        in_specs=[vmem, vmem, smem, vmem, vmem, vmem, vmem, vmem, smem] + [vmem] * 6,
        out_specs=(vmem,) * 3,
        scratch_shapes=scratch,
        compiler_params=pltpu.CompilerParams(
            collective_id=0, has_side_effects=True, vmem_limit_bytes=67043328
        ),
        name="step",
    )(
        noisy_state,
        target_state,
        noise_level,
        var_weight.reshape(1, VARS),
        embed_in,
        embed_out,
        norm_gain.reshape(1, D),
        qkv_weight,
        head_scale,
        out_weight,
        dec_weight,
        g2m_node.reshape(1, G_DEV),
        m2g_node.reshape(1, G_DEV),
        neighbours.T,
        lat_weight.reshape(1, G_DEV),
    )
    return dec[0, 127] / GRID, dec[:, :VARS], grad_out, grad_value


def solution(mesh):
    in_specs = (
        P(("chan", "member"), None, "band"),
        P(("chan", "member"), None, "band"),
        P(("chan", "member")),
        P(),
        P(),
        P(),
        P(),
        P(),
        P(),
        P(),
        P(),
        P("band"),
        P("band"),
        P("band", None),
    )
    out_specs = (P(), P(), P(), P())
    return jax.shard_map(local, mesh=mesh, in_specs=in_specs, out_specs=out_specs, check_vma=False)
```

```python
import math

import jax
import jax.numpy as jnp
from jax import lax
from jax.experimental import pallas as pl
from jax.experimental.pallas import tpu as pltpu
from jax.sharding import PartitionSpec as P

D = 512
VARS = 84
HEADS = 4
NBR = 32
G_DEV = 2048
M_DEV = 512
HEAD_DIM = 128
GRID = 32768
MEMBERS = 8
WINDOW = 3 * M_DEV
ROWS = 96
BF16, F32, I32 = jnp.bfloat16, jnp.float32, jnp.int32
MESH_ID = pl.DeviceIdType.MESH
UNITS = (
    ("out", 0, 1024, ("x", "z", "y")),
    ("out", 1024, 1024, ("x", "y", "z")),
    ("dec", 0, 512, ("x", "z", "y")),
    ("value", 0, 512, ("z", "y", "x")),
    ("value", 512, 512, ("y", "z", "x")),
    ("value", 1024, 512, ("z", "y", "x")),
    ("value", 1536, 512, ("y", "z", "x")),
)


def coordinates():
    band, chan, core = (lax.axis_index("band"), lax.axis_index("chan"), lax.axis_index("member"))
    return {"band": band, "x": chan, "y": lax.rem(band, 4), "z": band // 4, "core": core}


def peer_on(axis, at, step):
    other = lax.rem(at[axis] + step, 4)
    if axis == "x":
        return (at["band"], other, at["core"])
    if axis == "y":
        return (at["z"] * 4 + other, at["x"], at["core"])
    return (other * 4 + at["y"], at["x"], at["core"])


def sibling(at):
    return (at["band"], at["x"], 1 - at["core"])


class Flight:
    def __init__(self, copies, index, size_ref, device):
        self.whole = pltpu.make_async_remote_copy(
            src_ref=size_ref,
            dst_ref=size_ref,
            send_sem=copies.send_sems.at[index],
            recv_sem=copies.recv_sems.at[index],
            device_id=device,
            device_id_type=MESH_ID,
        )

    def wait_recv(self):
        self.whole.wait_recv()

    def wait_send(self):
        self.whole.wait_send()


class Copies:
    def __init__(self, send_sems, recv_sems):
        self.send_sems, self.recv_sems, self.all = send_sems, recv_sems, []

    def start(self, size_ref, group):
        index = len(self.all)
        for source, target, device in group:
            pltpu.make_async_remote_copy(
                src_ref=source,
                dst_ref=target,
                send_sem=self.send_sems.at[index],
                recv_sem=self.recv_sems.at[index],
                device_id=device,
                device_id_type=MESH_ID,
            ).start()
        self.all.append(Flight(self, index, size_ref, group[0][2]))
        return self.all[-1]


def greet(devices):
    for device in devices:
        pl.semaphore_signal(
            pltpu.get_barrier_semaphore(), inc=1, device_id=device, device_id_type=MESH_ID
        )


def await_greetings(devices):
    pl.semaphore_wait(pltpu.get_barrier_semaphore(), len(devices))


def sum_partners(at):
    return [sibling(at)] + [peer_on(axis, at, step) for axis in ("x", "y", "z") for step in (1, 2, 3)]


def sum_scratch(rows):
    half = rows // 2
    return [
        pltpu.VMEM((half, 128), F32),
        pltpu.VMEM((half, 128), F32),
        pltpu.VMEM((3, half // 4, 128), F32),
        pltpu.VMEM((half // 4, 128), F32),
        pltpu.VMEM((3, half // 16, 128), F32),
        pltpu.VMEM((4, half // 16, 128), F32),
        pltpu.VMEM((half // 16, 128), F32),
    ]


def device_sum(part, total, unit, refs, copies, at):
    near, pair, first_in, first, second_in, slots, second = refs
    origin, size_all, (first_axis, second_axis, third_axis) = unit[1:]
    half = size_all // 2
    quarter, tiny = half // 4, half // 16

    def rows(start, size):
        return pl.ds(pl.multiple_of(start, size), size)

    def scatter(source, landing, size, axis):
        group = []
        for step in (1, 2, 3):
            block = source.at[rows(lax.rem(at[axis] + step, 4) * size, size), :]
            group.append((block, landing.at[step - 1], peer_on(axis, at, step)))
        return copies.start(landing, group)

    def gather_sum(source, landing, size, axis, flight):
        flight.wait_recv()
        return (source[rows(at[axis] * size, size), :] + landing[0]) + (landing[1] + landing[2])

    def spread(start, size, axis):
        block = total.at[rows(start, size), :]
        return copies.start(
            total.at[rows(0, 3 * size), :], [(block, block, peer_on(axis, at, step)) for step in (1, 2, 3)]
        )

    mine = origin + at["core"] * half
    flight = copies.start(
        near, [(part.at[rows(origin + (1 - at["core"]) * half, half), :], near, sibling(at))]
    )
    yield
    flight.wait_recv()
    pair[...] = part[rows(mine, half), :] + near[...]
    flight = scatter(pair, first_in, quarter, first_axis)
    yield
    first[...] = gather_sum(pair, first_in, quarter, first_axis, flight)
    flight = scatter(first, second_in, tiny, second_axis)
    yield
    second[...] = gather_sum(first, second_in, tiny, second_axis, flight)
    slots[at[third_axis]] = second[...]
    flight = copies.start(
        slots.at[pl.ds(0, 3)],
        [(second, slots.at[at[third_axis]], peer_on(third_axis, at, step)) for step in (1, 2, 3)],
    )
    yield
    flight.wait_recv()
    outer = mine + at[first_axis] * quarter
    inner = outer + at[second_axis] * tiny
    total[rows(inner, tiny), :] = (slots[0] + slots[1]) + (slots[2] + slots[3])
    flight = spread(inner, tiny, second_axis)
    yield
    flight.wait_recv()
    flight = spread(outer, quarter, first_axis)
    yield
    flight.wait_recv()
    block = total.at[rows(mine, half), :]
    flight = copies.start(block, [(block, block, sibling(at))])
    yield
    flight.wait_recv()
    yield


def dot(left, right):
    return jnp.dot(left, right, preferred_element_type=F32)


def dot_t(left, right):
    return lax.dot_general(left, right, (((1,), (1,)), ((), ())), preferred_element_type=F32)


def pieces_of(values, count):
    pieces, rest = ([], values)
    for index in range(count):
        piece = rest.astype(BF16)
        pieces.append(piece)
        if index + 1 < count:
            rest = rest - piece.astype(F32)
    return pieces


def column_of(row, size):
    tall = jnp.transpose(jnp.broadcast_to(row, (128, size)))
    return tall


def unit_heads(values, width):
    split = values.reshape(HEADS, HEAD_DIM, width)
    scale = lax.rsqrt(jnp.mean(split * split, axis=1, keepdims=True) + 1e-06)
    return (split * scale).reshape(D, width)


def lanes(values, width):
    return jnp.concatenate([values] * (width // 128), axis=1)


class Phase:
    def __init__(self):
        self.scope = None

    def __call__(self, name):
        if self.scope is not None:
            self.scope.__exit__(None, None, None)
        self.scope = None if name is None else jax.named_scope(name)
        if self.scope is not None:
            self.scope.__enter__()


STEP_VMEM = 57 << 20
INPUTS = (
    ("noisy", (VARS, G_DEV), BF16),
    ("g2m", (1, G_DEV), I32),
    ("embed_in", (VARS, D), BF16),
    ("embed_out", (D, D), BF16),
    ("gain", (1, D), F32),
    ("qkv", (3, D, D), BF16),
    ("nbr", (NBR, M_DEV), I32),
    ("m2g", (1, G_DEV), I32),
    ("out_w", (D, D), BF16),
    ("dec_w", (VARS, D), BF16),
    ("target", (VARS, G_DEV), BF16),
    ("var", (1, VARS), F32),
)

SCRATCH = (
    ("state_in", (2, VARS, G_DEV), BF16),
    ("g2m_in", (2, 1, G_DEV), I32),
    ("pad_in", (128, D), BF16),
    ("embed_in_t", (D, 128), BF16),
    ("dec_t", (128, D), BF16),
    ("dec_full", (D, 128), BF16),
    ("embed_out_t", (D, D), BF16),
    ("q_t", (D, D), BF16),
    ("k_t", (D, D), BF16),
    ("v_t", (D, D), BF16),
    ("out_t", (D, D), BF16),
    ("node_hidden", (D, M_DEV), F32),
    ("mesh_in", (D, M_DEV), F32),
    ("normed", (D, M_DEV), BF16),
    ("normed_in", (D, 2 * M_DEV), BF16),
    ("unit_q", (D, M_DEV), BF16),
    ("unit_k", (WINDOW, D), BF16),
    ("values", (D, WINDOW), BF16),
    ("counts", (WINDOW, M_DEV), F32),
    ("counts_16", (WINDOW, M_DEV), BF16),
    ("exps", (HEADS, WINDOW, M_DEV), F32),
    ("probs", (HEADS, WINDOW, M_DEV), BF16),
    ("attended", (D, M_DEV), BF16),
    ("mesh_out", (D, M_DEV), BF16),
    ("table", (WINDOW, G_DEV), BF16),
    ("vars_own", (ROWS, M_DEV), F32),
    ("vars_two", (2 * ROWS, M_DEV), BF16),
    ("vars_out", (ROWS, M_DEV), BF16),
    ("vars_in", (ROWS, 2 * M_DEV), BF16),
    ("net", (ROWS, G_DEV), F32),
    ("weights", (VARS, G_DEV), F32),
    ("grad_net", (ROWS, G_DEV), BF16),
    ("node_out", (2, ROWS, M_DEV), BF16),
    ("node_in", (2, ROWS, M_DEV), BF16),
    ("node_own", (ROWS, M_DEV), F32),
    ("mesh_grad", (D, M_DEV), BF16),
    ("head_grad", (D, M_DEV), BF16),
    ("value_out", (2, D, M_DEV), BF16),
    ("value_in", (2, D, M_DEV), BF16),
    ("value_own", (D, M_DEV), F32),
    ("part_out", (2048, 128), F32),
    ("part_value", (2048, 128), F32),
    ("part_dec", (512, 128), F32),
)


def step_kernel(level_ref, head_scale_ref, *refs):
    hbm, (total_out, total_value, total_dec) = refs[: len(INPUTS)], refs[len(INPUTS) : len(INPUTS) + 3]
    scratch = refs[len(INPUTS) + 3 :]
    send_sems, recv_sems, load_sems = scratch[:3]
    held = dict(zip([name for name, shape, kind in INPUTS + SCRATCH], scratch[3:]))
    unit_refs = scratch[3 + len(INPUTS + SCRATCH) :]
    noisy_ref, g2m_ref, embed_in_ref, embed_out_ref = [
        held[name] for name in ("noisy", "g2m", "embed_in", "embed_out")
    ]
    gain_ref, qkv_ref, nbr_ref, m2g_ref = [held[name] for name in ("gain", "qkv", "nbr", "m2g")]
    out_w_ref, dec_w_ref, target_ref, var_ref = [held[name] for name in ("out_w", "dec_w", "target", "var")]
    (
        state_in,
        g2m_in,
        pad_in,
        embed_in_t,
        dec_t,
        dec_full,
        embed_out_t,
        q_t,
        k_t,
        v_t,
        out_t,
        node_hidden,
        mesh_in,
        normed,
        normed_in,
        unit_q,
        unit_k,
        values,
        counts,
        counts_16,
        exps,
        probs,
        attended,
        mesh_out,
        table,
        vars_own,
        vars_two,
        vars_out,
        vars_in,
        net,
        weights_ref,
        grad_net,
        node_out,
        node_in,
        node_own,
        mesh_grad,
        head_grad,
        value_out,
        value_in,
        value_own,
        part_out,
        part_value,
        part_dec,
    ) = [held[name] for name, shape, kind in SCRATCH]
    parts = {"out": part_out, "value": part_value, "dec": part_dec}
    totals = {"out": total_out, "value": total_value, "dec": total_dec}
    at = coordinates()
    band = at["band"]
    left = (lax.rem(band + 15, 16), at["x"], at["core"])
    right = (lax.rem(band + 1, 16), at["x"], at["core"])
    sides = ((0, left, 1), (1, right, 0))
    base = band * M_DEV
    copies = Copies(send_sems, recv_sems)
    phase = Phase()
    phase("greet")
    partners = [left, right] + sum_partners(at)
    greet(partners)
    loads = {}
    for index, (name, shape, kind) in enumerate(INPUTS):
        source = hbm[index].at[0] if name in ("noisy", "target") else hbm[index]
        loads[name] = pltpu.make_async_copy(source, held[name], load_sems.at[index])
        loads[name].start()
    loads["noisy"].wait()
    loads["g2m"].wait()
    await_greetings(partners)

    phase("sendstate")
    node_flight = copies.start(g2m_in, [(g2m_ref, g2m_in.at[slot], device) for side, device, slot in sides])
    state_flights = []
    for chunk in range(4):
        cells = pl.ds(512 * chunk, 512)
        state_flights.append(
            copies.start(
                state_in.at[:, :, cells],
                [
                    (noisy_ref.at[:, cells], state_in.at[slot, :, cells], device)
                    for side, device, slot in sides
                ],
            )
        )

    phase("transposes")
    loads["embed_in"].wait()
    pad_in[...] = jnp.zeros_like(pad_in)
    pad_in[:VARS, :] = embed_in_ref[...]
    embed_in_t[...] = jnp.transpose(pad_in[...])
    level = jnp.full((1, 1), level_ref[0], F32)
    level_sq = level * level + 1.0
    scale_in = lax.rsqrt(level_sq)
    skip_scale = 1.0 / level_sq
    out_scale = level * scale_in
    half_scale = 0.5 * scale_in

    def encode(state, nodes):
        half_t = dot(embed_in_t[:, :VARS], state) * half_scale
        hidden = (half_t + half_t * jnp.tanh(half_t)).astype(BF16)
        ids = lax.broadcasted_iota(I32, (M_DEV, 512), 0)
        chosen = jnp.where(nodes - base == ids, 1.0, 0.0).astype(BF16)
        node_hidden[...] += dot_t(hidden, chosen)

    phase("encodeown")
    node_hidden[...] = jnp.zeros_like(node_hidden)

    @pl.loop(0, 4)
    def _(chunk):
        cells = pl.ds(pl.multiple_of(chunk * 512, 512), 512)
        encode(noisy_ref[:, cells], g2m_ref[:, cells])

    loads["embed_out"].wait()
    embed_out_t[...] = jnp.transpose(embed_out_ref[...])
    phase("encodehalo")
    node_flight.wait_recv()
    for chunk in range(4):
        cells = slice(512 * chunk, 512 * chunk + 512)
        state_flights[chunk].wait_recv()

        @pl.loop(0, 2)
        def _(slot):
            encode(state_in[slot, :, cells], g2m_in[slot, :, cells])

    phase("embedout")
    encoded = None
    for piece in pieces_of(node_hidden[...], 3):
        term = dot(embed_out_t[...], piece)
        encoded = term if encoded is None else encoded + term
    mesh_in[...] = encoded
    mean_sq = jnp.mean(encoded * encoded, axis=0, keepdims=True)
    loads["gain"].wait()
    gain = lanes(column_of(gain_ref[...], D), M_DEV)
    normed[...] = (encoded * lax.rsqrt(mean_sq + 1e-05) * gain).astype(BF16)

    normed_flights = []
    for chunk in range(4):
        nodes = pl.ds(128 * chunk, 128)
        normed_flights.append(
            copies.start(
                normed_in.at[:, pl.ds(256 * chunk, 256)],
                [
                    (normed.at[:, nodes], normed_in.at[:, pl.ds(256 * chunk + 128 * slot, 128)], device)
                    for side, device, slot in sides
                ],
            )
        )

    phase("queries")
    loads["qkv"].wait()
    q_t[...] = jnp.transpose(qkv_ref[0])
    k_t[...] = jnp.transpose(qkv_ref[1])
    v_t[...] = jnp.transpose(qkv_ref[2])
    unit_q[...] = unit_heads(dot(q_t[...], normed[...]), M_DEV).astype(BF16)

    def attend(near, start, width):
        keys = unit_heads(dot(k_t[...], near), width).astype(BF16)
        unit_k[start : start + width, :] = jnp.transpose(keys)
        values[:, start : start + width] = dot(v_t[...], near).astype(BF16)
        sums_now = []
        count = counts[start : start + width, :]
        for head in range(HEADS):
            part = slice(HEAD_DIM * head, HEAD_DIM * head + HEAD_DIM)
            scores = dot(unit_k[start : start + width, part], unit_q[part, :])
            exp = jnp.exp(scores * (head_scale_ref[head] / HEAD_DIM))
            exps[head, start : start + width, :] = exp
            sums_now.append(jnp.sum(exp * count, axis=0, keepdims=True))
        return sums_now

    phase("counts")
    loads["nbr"].wait()
    @pl.loop(0, 8)
    def _(block):
        ids = lax.broadcasted_iota(I32, (64, M_DEV), 0) + block * 64
        total = jnp.zeros((64, M_DEV), I32)
        for j in range(NBR):
            near = nbr_ref[j : j + 1, :] - (base - M_DEV)
            patch = near // M_DEV
            within = near - patch * M_DEV
            field = jnp.where(patch == 0, 64, jnp.where(patch == 1, 1, 4096))
            total = total + jnp.where(within == ids, field, 0)
        chunk = block // 2
        part = (block - 2 * chunk) * 64
        for start, shift in (
            (block * 64, 0),
            (M_DEV + 256 * chunk + part, 6),
            (M_DEV + 256 * chunk + 128 + part, 12),
        ):
            count = lax.shift_right_logical(total, jnp.full_like(total, shift)) & 63
            rows = pl.ds(pl.multiple_of(start, 64), 64)
            counts[rows, :] = count.astype(F32)
            counts_16[rows, :] = count.astype(F32).astype(BF16)

    phase("table")
    loads["m2g"].wait()
    for block in range(12):
        if block < 4:
            offset = 128 * block
        else:
            offset = 128 * ((block - 4) // 2) + (M_DEV if (block - 4) % 2 else -M_DEV)
        ids = lax.broadcasted_iota(I32, (128, G_DEV), 0) + (base + offset)
        table[128 * block : 128 * block + 128, :] = jnp.where(m2g_ref[...] == ids, 1.0, 0.0).astype(BF16)

    phase("weights")
    loads["var"].wait()
    cells = lax.broadcasted_iota(I32, (1, G_DEV), 1) + band * G_DEV
    lat_weight = 0.2 + jnp.cos(math.pi * (cells.astype(F32) + 0.5) / GRID - 0.5 * math.pi)
    square = lax.broadcasted_iota(I32, (VARS, VARS), 0) == lax.broadcasted_iota(I32, (VARS, VARS), 1)
    var_column = jnp.sum(jnp.where(square, var_ref[...], 0.0), axis=1, keepdims=True)
    weights_ref[...] = var_column * lat_weight
    loads["out_w"].wait()
    loads["dec_w"].wait()
    out_t[...] = jnp.transpose(out_w_ref[...])
    dec_t[...] = jnp.zeros_like(dec_t)
    dec_t[:VARS, :] = dec_w_ref[...]
    dec_full[...] = jnp.transpose(dec_t[...])
    loads["target"].wait()
    phase("scores")
    exp_sums = None
    for chunk in range(6):
        if chunk < 2:
            near = normed[:, 256 * chunk : 256 * chunk + 256]
        else:
            normed_flights[chunk - 2].wait_recv()
            near = normed_in[:, 256 * (chunk - 2) : 256 * (chunk - 2) + 256]
        sums_now = attend(near, 256 * chunk, 256)
        exp_sums = sums_now if exp_sums is None else [a + b for a, b in zip(exp_sums, sums_now)]

    phase("probs")
    for head in range(HEADS):
        inverse = 1.0 / exp_sums[head]
        part = slice(HEAD_DIM * head, HEAD_DIM * head + HEAD_DIM)

        @pl.loop(0, 6)
        def _(block):
            rows = pl.ds(pl.multiple_of(block * 256, 256), 256)
            prob = (exps[head, rows, :] * inverse).astype(BF16)
            probs[head, rows, :] = prob * counts_16[rows, :]

        attended[part, :] = dot(values[part, :], probs[head]).astype(BF16)

    phase("meshout")
    mesh_out[...] = (mesh_in[...] + dot(out_t[...], attended[...])).astype(BF16)
    vars_own[...] = dot(dec_t[:ROWS, :], mesh_out[...])
    vars_out[...] = vars_own[...].astype(BF16)
    vars_flight = copies.start(
        vars_in,
        [
            (
                vars_out.at[:, pl.ds(128 * chunk, 128)],
                vars_in.at[:, pl.ds(256 * chunk + 128 * slot, 128)],
                device,
            )
            for chunk in range(4)
            for side, device, slot in sides
        ],
    )

    phase("decodeown")
    for index, piece in enumerate(pieces_of(vars_own[...], 2)):
        vars_two[ROWS * index : ROWS * index + ROWS, :] = piece

    @pl.loop(0, 4)
    def _(chunk):
        cells = pl.ds(pl.multiple_of(chunk * 512, 512), 512)
        both = dot(vars_two[...], table[:M_DEV, cells])
        net[:, cells] = both[:ROWS, :] + both[ROWS:, :]

    phase("waitvars")
    vars_flight.wait_recv()
    phase("decodehalo")

    @pl.loop(0, 4)
    def _(chunk):
        cells = pl.ds(pl.multiple_of(chunk * 512, 512), 512)
        net[:, cells] = net[:, cells] + dot(vars_in[...], table[M_DEV:, cells])

    phase("errors")
    weights = weights_ref[...]
    errors = (
        skip_scale * noisy_ref[...].astype(F32) + out_scale * net[:VARS, :] - target_ref[...].astype(F32)
    )
    scale_all = 1.0 / (MEMBERS * VARS)
    loss = jnp.sum(jnp.sum(weights * errors * errors, axis=1, keepdims=True), axis=0, keepdims=True) * scale_all
    grad_net[...] = jnp.zeros_like(grad_net)
    grad_net[:VARS, :] = ((2.0 * out_scale * scale_all) * weights * errors).astype(BF16)

    phase("nodepart")
    node_part = dot_t(grad_net[...], table[M_DEV:, :])
    for chunk in range(4):
        for side in (0, 1):
            start = 256 * chunk + 128 * side
            node_out[side, :, 128 * chunk : 128 * chunk + 128] = node_part[:, start : start + 128].astype(BF16)
    node_flight = copies.start(
        node_in, [(node_out.at[side], node_in.at[slot], device) for side, device, slot in sides]
    )
    phase("nodeown")
    node_own[...] = dot_t(grad_net[...], table[:M_DEV, :])
    phase("waitnode")
    node_flight.wait_recv()
    node_grad = node_own[...] + node_in[0].astype(F32) + node_in[1].astype(F32)
    phase("meshgrad")
    node_pieces = pieces_of(node_grad, 3)
    grown = None
    for piece in node_pieces:
        term = dot(dec_full[:, :ROWS], piece)
        grown = term if grown is None else grown + term
    mesh_grad[...] = grown.astype(BF16)
    head_grad[...] = dot(out_w_ref[...], mesh_grad[...]).astype(BF16)

    phase("valuerim")
    value_flights = []
    for head in range(HEADS):
        part = slice(HEAD_DIM * head, HEAD_DIM * head + HEAD_DIM)
        spread = dot_t(head_grad[part, :], probs[head, M_DEV:, :])
        for chunk in range(4):
            for side in (0, 1):
                start = 256 * chunk + 128 * side
                value_out[side, part, 128 * chunk : 128 * chunk + 128] = spread[
                    :, start : start + 128
                ].astype(BF16)
        rows = pl.ds(HEAD_DIM * head, HEAD_DIM)
        value_flights.append(
            copies.start(
                value_in.at[:, rows, :],
                [
                    (value_out.at[side, rows, :], value_in.at[slot, rows, :], device)
                    for side, device, slot in sides
                ],
            )
        )

    phase("gradout")
    units = []
    for index, unit in enumerate(UNITS):
        name = unit[0]
        units.append(
            device_sum(parts[name], totals[name], unit, unit_refs[7 * index : 7 * index + 7], copies, at)
        )
    out_units, value_units = (units[:3], units[3:])
    out_sum = dot_t(attended[...], mesh_grad[...])
    for lane in range(4):
        part_out[512 * lane : 512 * lane + 512, :] = out_sum[:, 128 * lane : 128 * lane + 128]
    for unit in out_units[:2]:
        next(unit)
    dec_sum = None
    for piece in node_pieces:
        term = dot_t(piece, mesh_out[...])
        dec_sum = term if dec_sum is None else dec_sum + term
    for lane in range(4):
        part_dec[ROWS * lane : ROWS * lane + ROWS, :] = dec_sum[:, 128 * lane : 128 * lane + 128]
    part_dec[4 * ROWS :, :] = jnp.broadcast_to(loss, (128, 128))
    next(out_units[2])
    phase("valueown")
    for head in range(HEADS):
        part = slice(HEAD_DIM * head, HEAD_DIM * head + HEAD_DIM)
        value_own[part, :] = dot_t(head_grad[part, :], probs[head, :M_DEV, :])

    def advance(some):
        for unit in some:
            next(unit, None)

    def finish_head(head):
        phase("gradvalue%d" % head)
        part = slice(HEAD_DIM * head, HEAD_DIM * head + HEAD_DIM)
        value_flights[head].wait_recv()
        grad = value_own[part, :] + value_in[0, part, :].astype(F32) + value_in[1, part, :].astype(F32)
        part_value[512 * head : 512 * head + 512, :] = dot_t(normed[...], grad.astype(BF16))
        next(value_units[head])

    advance(out_units)
    finish_head(0)
    advance(value_units[:1])
    finish_head(1)
    advance(value_units[1:2])
    finish_head(2)
    advance(value_units[2:3])
    finish_head(3)
    advance(out_units)
    advance(value_units[3:])
    for turn in range(6):
        phase("turn%d" % turn)
        advance(value_units + out_units)
    phase("drain")
    for copy in copies.all:
        copy.wait_send()
    phase(None)


def finish_kernel(out_ref, value_ref, dec_ref, out_hbm, value_hbm, dec_result, loss_result, sems):
    flights = []
    for index, (source, target) in enumerate(((out_ref, out_hbm), (value_ref, value_hbm))):
        for lane in range(4):
            flights.append(
                pltpu.make_async_copy(
                    source.at[pl.ds(512 * lane, 512), :],
                    target.at[:, pl.ds(128 * lane, 128)],
                    sems.at[4 * index + lane],
                )
            )
            flights[-1].start()
    for lane in range(4):
        dec_result[:, 128 * lane : 128 * lane + 128] = dec_ref[ROWS * lane : ROWS * lane + VARS, :]
    loss_result[...] = dec_ref[4 * ROWS : 4 * ROWS + 1, :1] / GRID
    for flight in flights:
        flight.wait()


def local(
    noisy_state,
    target_state,
    noise_level,
    var_weight,
    embed_in,
    embed_out,
    norm_gain,
    qkv_weight,
    head_scale,
    out_weight,
    dec_weight,
    g2m_node,
    m2g_node,
    neighbours,
):
    vmem = pl.BlockSpec(memory_space=pltpu.VMEM)
    smem = pl.BlockSpec(memory_space=pltpu.SMEM)
    anywhere = pl.BlockSpec(memory_space=pl.ANY)
    copies = 15 + 7 * len(UNITS)
    scratch = [pltpu.SemaphoreType.DMA((copies,))] * 2 + [pltpu.SemaphoreType.DMA((len(INPUTS),))]
    scratch += [pltpu.VMEM(shape, kind) for name, shape, kind in INPUTS + SCRATCH]
    for unit in UNITS:
        scratch += sum_scratch(unit[2])
    totals = pl.pallas_call(
        step_kernel,
        out_shape=[pltpu.VMEM((rows, 128), F32) for rows in (2048, 2048, 512)],
        in_specs=[smem, smem] + [anywhere] * len(INPUTS),
        out_specs=[vmem] * 3,
        scratch_shapes=scratch,
        compiler_params=pltpu.CompilerParams(
            collective_id=0, has_side_effects=True, vmem_limit_bytes=STEP_VMEM
        ),
        name="step",
    )(
        noise_level,
        head_scale,
        noisy_state,
        g2m_node.reshape(1, G_DEV),
        embed_in,
        embed_out,
        norm_gain.reshape(1, D),
        qkv_weight,
        neighbours.T,
        m2g_node.reshape(1, G_DEV),
        out_weight,
        dec_weight.T,
        target_state,
        var_weight.reshape(1, VARS),
    )
    square = jax.ShapeDtypeStruct((D, D), F32)
    grad_out, grad_value, dec, loss = pl.pallas_call(
        finish_kernel,
        out_shape=(square, square, jax.ShapeDtypeStruct((VARS, D), F32), jax.ShapeDtypeStruct((1, 1), F32)),
        in_specs=[vmem] * 3,
        out_specs=(anywhere, anywhere, vmem, vmem),
        scratch_shapes=[pltpu.SemaphoreType.DMA((8,))],
        compiler_params=pltpu.CompilerParams(vmem_limit_bytes=8 << 20),
        name="finish",
    )(*totals)
    return loss.reshape(()), dec.T, grad_out, grad_value


def solution(mesh):
    in_specs = (
        P(("chan", "member"), None, "band"),
        P(("chan", "member"), None, "band"),
        P(("chan", "member")),
        P(),
        P(),
        P(),
        P(),
        P(),
        P(),
        P(),
        P(),
        P("band"),
        P("band"),
        P("band", None),
    )
    out_specs = (P(), P(), P(), P())
    return jax.shard_map(local, mesh=mesh, in_specs=in_specs, out_specs=out_specs, check_vma=False)
```

```python
import math

import jax
import jax.numpy as jnp
from jax import lax
from jax.experimental import pallas as pl
from jax.experimental.pallas import tpu as pltpu
from jax.sharding import PartitionSpec as P

D = 512
VARS = 84
HEADS = 4
NBR = 32
G_DEV = 2048
M_DEV = 512
HEAD_DIM = 128
GRID = 32768
MEMBERS = 8
WINDOW = 3 * M_DEV
ROWS = 96
BF16, F32, I32 = jnp.bfloat16, jnp.float32, jnp.int32
MESH_ID = pl.DeviceIdType.MESH
UNITS = (
    (0, 0, 768, 0, 0, "xyz"),
    (0, 768, 768, 0, 1, "yzx"),
    (0, 1536, 512, 1, 0, "zxy"),
    (2, 0, 512, 4, 0, "zxy"),
    (1, 0, 768, 2, 0, "xyz"),
    (1, 768, 768, 2, 1, "yzx"),
    (1, 1536, 512, 3, 0, "zxy"),
)
TOTALS = ((4, 4, 96, 128), (2, 4, 64, 128), (4, 4, 96, 128), (2, 4, 64, 128), (2, 4, 64, 128))


def coordinates():
    band, chan, core = (lax.axis_index("band"), lax.axis_index("chan"), lax.axis_index("member"))
    return {"band": band, "x": chan, "y": lax.rem(band, 4), "z": band // 4, "core": core}


def peer_on(axis, at, step):
    other = lax.rem(at[axis] + step, 4)
    if axis == "x":
        return (at["band"], other, at["core"])
    if axis == "y":
        return (at["z"] * 4 + other, at["x"], at["core"])
    return (other * 4 + at["y"], at["x"], at["core"])


def sibling(at):
    return (at["band"], at["x"], 1 - at["core"])


class Flight:
    def __init__(self, copies, index, size_ref, device):
        self.whole = pltpu.make_async_remote_copy(
            src_ref=size_ref,
            dst_ref=size_ref,
            send_sem=copies.send_sems.at[index],
            recv_sem=copies.recv_sems.at[index],
            device_id=device,
            device_id_type=MESH_ID,
        )

    def wait_recv(self):
        self.whole.wait_recv()

    def wait_send(self):
        self.whole.wait_send()


class Copies:
    def __init__(self, send_sems, recv_sems):
        self.send_sems, self.recv_sems, self.all = send_sems, recv_sems, []

    def start(self, size_ref, group):
        index = len(self.all)
        for source, target, device in group:
            pltpu.make_async_remote_copy(
                src_ref=source,
                dst_ref=target,
                send_sem=self.send_sems.at[index],
                recv_sem=self.recv_sems.at[index],
                device_id=device,
                device_id_type=MESH_ID,
            ).start()
        self.all.append(Flight(self, index, size_ref, group[0][2]))
        return self.all[-1]


def greet(devices):
    for device in devices:
        pl.semaphore_signal(
            pltpu.get_barrier_semaphore(), inc=1, device_id=device, device_id_type=MESH_ID
        )


def await_greetings(devices):
    pl.semaphore_wait(pltpu.get_barrier_semaphore(), len(devices))


def sum_partners(at):
    return [sibling(at)] + [peer_on(axis, at, step) for axis in ("x", "y", "z") for step in (1, 2, 3)]


def sum_scratch(rows):
    half = rows // 2
    return [
        pltpu.VMEM((half, 128), F32),
        pltpu.VMEM((half, 128), F32),
        pltpu.VMEM((3, half // 4, 128), F32),
        pltpu.VMEM((half // 4, 128), F32),
        pltpu.VMEM((3, half // 16, 128), F32),
        pltpu.VMEM((4, half // 16, 128), F32),
        pltpu.VMEM((half // 16, 128), F32),
    ]


def device_sum(part, total, unit, refs, copies, at):
    near, pair, first_in, first, second_in, slots, second = refs
    origin, size_all, which, place, (first_axis, second_axis, third_axis) = unit[1:]
    half = size_all // 2
    quarter, tiny = half // 4, half // 16

    def rows(start, size):
        return pl.ds(pl.multiple_of(start, size), size)

    def scatter(source, landing, size, axis):
        group = []
        for step in (1, 2, 3):
            block = source.at[rows(lax.rem(at[axis] + step, 4) * size, size), :]
            group.append((block, landing.at[step - 1], peer_on(axis, at, step)))
        return copies.start(landing, group)

    def gather_sum(source, landing, size, axis, flight):
        flight.wait_recv()
        return (source[rows(at[axis] * size, size), :] + landing[0]) + (landing[1] + landing[2])

    mine = origin + at["core"] * half
    flight = copies.start(
        near, [(part.at[rows(origin + (1 - at["core"]) * half, half), :], near, sibling(at))]
    )
    yield
    flight.wait_recv()
    pair[...] = part[rows(mine, half), :] + near[...]
    flight = scatter(pair, first_in, quarter, first_axis)
    yield
    first[...] = gather_sum(pair, first_in, quarter, first_axis, flight)
    flight = scatter(first, second_in, tiny, second_axis)
    yield
    second[...] = gather_sum(first, second_in, tiny, second_axis, flight)
    slots[at[third_axis]] = second[...]
    flight = copies.start(
        slots.at[pl.ds(0, 3)],
        [(second, slots.at[at[third_axis]], peer_on(third_axis, at, step)) for step in (1, 2, 3)],
    )
    yield
    flight.wait_recv()
    block = 2 * place + at["core"]
    one = total.at[block, at[first_axis], rows(at[second_axis] * tiny, tiny), :]
    total[block, at[first_axis], rows(at[second_axis] * tiny, tiny), :] = (slots[0] + slots[1]) + (
        slots[2] + slots[3]
    )
    flight = copies.start(
        total.at[block, pl.ds(0, 3), rows(0, tiny), :],
        [(one, one, peer_on(first_axis, at, step)) for step in (1, 2, 3)],
    )
    yield
    flight.wait_recv()
    line = total.at[block, :, rows(at[second_axis] * tiny, tiny), :]
    flight = copies.start(
        total.at[block, :, pl.ds(0, 3 * tiny), :],
        [(line, line, peer_on(second_axis, at, step)) for step in (1, 2, 3)],
    )
    yield
    flight.wait_recv()
    flight = copies.start(total.at[block], [(total.at[block], total.at[block], sibling(at))])
    yield
    flight.wait_recv()
    yield


def dot(left, right):
    return jnp.dot(left, right, preferred_element_type=F32)


def dot_t(left, right):
    return lax.dot_general(left, right, (((1,), (1,)), ((), ())), preferred_element_type=F32)


def pieces_of(values, count):
    pieces, rest = ([], values)
    for index in range(count):
        piece = rest.astype(BF16)
        pieces.append(piece)
        if index + 1 < count:
            rest = rest - piece.astype(F32)
    return pieces


def column_of(row, size):
    tall = jnp.transpose(jnp.broadcast_to(row, (128, size)))
    return tall


def unit_heads(values, width):
    split = values.reshape(HEADS, HEAD_DIM, width)
    scale = lax.rsqrt(jnp.mean(split * split, axis=1, keepdims=True) + 1e-06)
    return (split * scale).reshape(D, width)


def lanes(values, width):
    return jnp.concatenate([values] * (width // 128), axis=1)


STEP_VMEM = 59 << 20
CHUNKS = ((0, 512), (512, 512), (1024, 512), (1536, 256), (1792, 256))
INPUTS = (
    ("noisy", (VARS, G_DEV), BF16),
    ("g2m", (1, G_DEV), I32),
    ("embed_in", (VARS, D), BF16),
    ("embed_out", (D, D), BF16),
    ("gain", (1, D), F32),
    ("qkv", (3, D, D), BF16),
    ("nbr", (NBR, M_DEV), I32),
    ("m2g", (1, G_DEV), I32),
    ("out_w", (D, D), BF16),
    ("dec_w", (VARS, D), BF16),
    ("target", (VARS, G_DEV), BF16),
    ("var", (1, VARS), F32),
    ("level", (1, 1), F32),
)

SCRATCH = (
    ((2, VARS, G_DEV), BF16),
    ((2, VARS, G_DEV), BF16),
    ((2, 1, G_DEV), I32),
    ((2, 1, G_DEV), I32),
    ((128, D), BF16),
    ((D, 128), BF16),
    ((128, D), BF16),
    ((D, 128), BF16),
    ((D, D), BF16),
    ((D, D), BF16),
    ((D, D), BF16),
    ((D, D), BF16),
    ((D, D), BF16),
    ((D, M_DEV), F32),
    ((D, M_DEV), F32),
    ((D, M_DEV), BF16),
    ((D, 2 * M_DEV), BF16),
    ((D, M_DEV), BF16),
    ((WINDOW, D), BF16),
    ((D, WINDOW), BF16),
    ((NBR, M_DEV), I32),
    ((NBR, M_DEV), I32),
    ((WINDOW, M_DEV), F32),
    ((WINDOW, M_DEV), BF16),
    ((HEADS, WINDOW, M_DEV), F32),
    ((HEADS, WINDOW, M_DEV), BF16),
    ((D, M_DEV), BF16),
    ((D, M_DEV), BF16),
    ((M_DEV, 3 * G_DEV), BF16),
    ((2 * ROWS, M_DEV), BF16),
    ((VARS, 3 * G_DEV), F32),
    ((ROWS, 3 * G_DEV), BF16),
    ((D, M_DEV), BF16),
    ((D, M_DEV), BF16),
    ((2048, 128), F32),
    ((2048, 128), F32),
    ((512, 128), F32),
)


def step_kernel(head_scale_ref, *refs):
    hbm, totals = refs[: len(INPUTS)], refs[len(INPUTS) : len(INPUTS) + len(TOTALS)]
    scratch = refs[len(INPUTS) + len(TOTALS) :]
    send_sems, recv_sems, load_sems = scratch[:3]
    held = dict(zip([name for name, shape, kind in INPUTS], scratch[3:]))
    unit_refs = scratch[3 + len(INPUTS + SCRATCH) :]
    (
        noisy_ref,
        g2m_ref,
        embed_in_ref,
        embed_out_ref,
        gain_ref,
        qkv_ref,
        nbr_ref,
        m2g_ref,
        out_w_ref,
        dec_w_ref,
        target_ref,
        var_ref,
        level_ref,
    ) = scratch[3 : 3 + len(INPUTS)]
    (
        state_in,
        target_in,
        g2m_in,
        m2g_in,
        pad_in,
        embed_in_t,
        dec_t,
        dec_full,
        embed_out_t,
        q_t,
        k_t,
        v_t,
        out_t,
        node_hidden,
        mesh_in,
        normed,
        normed_in,
        unit_q,
        unit_k,
        values,
        within,
        fields,
        counts,
        counts_16,
        exps,
        probs,
        attended,
        mesh_out,
        table,
        vars_two,
        weights_ref,
        grad_net,
        mesh_grad,
        head_grad,
        part_out,
        part_value,
        part_dec,
    ) = scratch[3 + len(INPUTS) : 3 + len(INPUTS + SCRATCH)]
    parts = (part_out, part_value, part_dec)
    at = coordinates()
    band = at["band"]
    left = (lax.rem(band + 15, 16), at["x"], at["core"])
    right = (lax.rem(band + 1, 16), at["x"], at["core"])
    sides = ((0, left, 1), (1, right, 0))
    base = band * M_DEV
    copies = Copies(send_sems, recv_sems)
    partners = [left, right] + sum_partners(at)
    greet(partners)
    loads = {}
    for index, (name, shape, kind) in enumerate(INPUTS):
        source = hbm[index].at[0] if name in ("noisy", "target") else hbm[index]
        loads[name] = pltpu.make_async_copy(source, held[name], load_sems.at[index])
        loads[name].start()
    loads["noisy"].wait()
    loads["g2m"].wait()
    await_greetings(partners)

    node_flight = copies.start(g2m_in, [(g2m_ref, g2m_in.at[slot], device) for side, device, slot in sides])
    state_flights = []
    for first, size in CHUNKS:
        cells = pl.ds(first, size)
        state_flights.append(
            copies.start(
                state_in.at[:, :, cells],
                [
                    (noisy_ref.at[:, cells], state_in.at[slot, :, cells], device)
                    for side, device, slot in sides
                ],
            )
        )


    def send_target(first, size):
        cells = pl.ds(first, size)
        return copies.start(
            target_in.at[:, :, cells],
            [(target_ref.at[:, cells], target_in.at[slot, :, cells], device) for side, device, slot in sides],
        )

    loads["m2g"].wait()
    cell_flight = copies.start(m2g_in, [(m2g_ref, m2g_in.at[slot], device) for side, device, slot in sides])
    loads["target"].wait()
    target_flights = [send_target(512 * chunk, 512) for chunk in range(3)]
    loads["embed_in"].wait()
    pad_in[...] = jnp.zeros_like(pad_in)
    pad_in[:VARS, :] = embed_in_ref[...]
    embed_in_t[...] = jnp.transpose(pad_in[...])
    loads["level"].wait()
    level = level_ref[...]
    level_sq = level * level + 1.0
    scale_in = lax.rsqrt(level_sq)
    skip_scale = 1.0 / level_sq
    out_scale = level * scale_in
    half_scale = 0.5 * scale_in

    def encode(state, nodes):
        half_t = dot(embed_in_t[:, :VARS], state) * half_scale
        hidden = (half_t + half_t * jnp.tanh(half_t)).astype(BF16)
        ids = lax.broadcasted_iota(I32, (M_DEV, state.shape[1]), 0)
        chosen = jnp.where(nodes - base == ids, 1.0, 0.0).astype(BF16)
        node_hidden[...] += dot_t(hidden, chosen)

    node_hidden[...] = jnp.zeros_like(node_hidden)

    @pl.loop(0, 4)
    def _(chunk):
        cells = pl.ds(pl.multiple_of(chunk * 512, 512), 512)
        encode(noisy_ref[:, cells], g2m_ref[:, cells])

    loads["embed_out"].wait()
    embed_out_t[...] = jnp.transpose(embed_out_ref[...])
    loads["var"].wait()
    square = lax.broadcasted_iota(I32, (VARS, VARS), 0) == lax.broadcasted_iota(I32, (VARS, VARS), 1)
    var_column = jnp.sum(jnp.where(square, var_ref[...], 0.0), axis=1, keepdims=True)

    def prepare(place, nodes):
        local = nodes - base
        ids = lax.broadcasted_iota(I32, (M_DEV, G_DEV), 0)
        block = slice(G_DEV * place, G_DEV * place + G_DEV)
        table[:, block] = jnp.where(local == ids, 1.0, 0.0).astype(BF16)
        cells = lax.broadcasted_iota(I32, (1, G_DEV), 1) + lax.rem(band + (0, 15, 1)[place], 16) * G_DEV
        lat_weight = 0.2 + jnp.cos(math.pi * (cells.astype(F32) + 0.5) / GRID - 0.5 * math.pi)
        mine = (local >= 0) & (local < M_DEV)
        weights_ref[:, block] = var_column * jnp.where(mine, lat_weight, 0.0)

    prepare(0, m2g_ref[...])
    node_flight.wait_recv()
    for (first, size), flight in zip(CHUNKS, state_flights):
        cells = slice(first, first + size)
        flight.wait_recv()

        for slot in range(2):
            encode(state_in[slot, :, cells], g2m_in[slot, :, cells])

    encoded = None
    for piece in pieces_of(node_hidden[...], 3):
        term = dot(embed_out_t[...], piece)
        encoded = term if encoded is None else encoded + term
    mesh_in[...] = encoded
    mean_sq = jnp.mean(encoded * encoded, axis=0, keepdims=True)
    loads["gain"].wait()
    gain = lanes(column_of(gain_ref[...], D), M_DEV)
    normed[...] = (encoded * lax.rsqrt(mean_sq + 1e-05) * gain).astype(BF16)

    normed_flights = []
    for chunk in range(4):
        nodes = pl.ds(128 * chunk, 128)
        normed_flights.append(
            copies.start(
                normed_in.at[:, pl.ds(256 * chunk, 256)],
                [
                    (normed.at[:, nodes], normed_in.at[:, pl.ds(256 * chunk + 128 * slot, 128)], device)
                    for side, device, slot in sides
                ],
            )
        )

    target_flights.append(send_target(1536, 512))

    loads["qkv"].wait()
    q_t[...] = jnp.transpose(qkv_ref[0])
    k_t[...] = jnp.transpose(qkv_ref[1])
    v_t[...] = jnp.transpose(qkv_ref[2])
    unit_q[...] = unit_heads(dot(q_t[...], normed[...]), M_DEV).astype(BF16)

    def attend(near, start, width):
        keys = unit_heads(dot(k_t[...], near), width).astype(BF16)
        unit_k[start : start + width, :] = jnp.transpose(keys)
        values[:, start : start + width] = dot(v_t[...], near).astype(BF16)
        sums_now = []
        count = counts[start : start + width, :]
        for head in range(HEADS):
            part = slice(HEAD_DIM * head, HEAD_DIM * head + HEAD_DIM)
            scores = dot(unit_k[start : start + width, part], unit_q[part, :])
            exp = jnp.exp(scores * (head_scale_ref[head] / HEAD_DIM))
            exps[head, start : start + width, :] = exp
            sums_now.append(jnp.sum(exp * count, axis=0, keepdims=True))
        return sums_now

    loads["nbr"].wait()
    window = nbr_ref[...] - (base - M_DEV)
    patch = lax.shift_right_arithmetic(window, jnp.full_like(window, 9))
    within[...] = window - patch * M_DEV
    fields[...] = jnp.where(patch == 0, 64, jnp.where(patch == 1, 1, 4096))

    @pl.loop(0, 8)
    def _(block):
        ids = lax.broadcasted_iota(I32, (64, M_DEV), 0) + block * 64
        total = jnp.zeros((64, M_DEV), I32)
        for j in range(NBR):
            total = total + jnp.where(within[j : j + 1, :] == ids, fields[j : j + 1, :], 0)
        chunk = block // 2
        part = (block - 2 * chunk) * 64
        for start, shift in (
            (block * 64, 0),
            (M_DEV + 256 * chunk + part, 6),
            (M_DEV + 256 * chunk + 128 + part, 12),
        ):
            count = lax.shift_right_logical(total, jnp.full_like(total, shift)) & 63
            rows = pl.ds(pl.multiple_of(start, 64), 64)
            counts[rows, :] = count.astype(F32)
            counts_16[rows, :] = count.astype(F32).astype(BF16)

    cell_flight.wait_recv()
    for slot in range(2):
        prepare(1 + slot, m2g_in[slot])

    loads["out_w"].wait()
    loads["dec_w"].wait()
    out_t[...] = jnp.transpose(out_w_ref[...])
    dec_t[...] = jnp.zeros_like(dec_t)
    dec_t[:VARS, :] = dec_w_ref[...]
    dec_full[...] = jnp.transpose(dec_t[...])
    exp_sums = None
    for chunk in range(6):
        if chunk < 2:
            near = normed[:, 256 * chunk : 256 * chunk + 256]
        else:
            normed_flights[chunk - 2].wait_recv()
            near = normed_in[:, 256 * (chunk - 2) : 256 * (chunk - 2) + 256]
        sums_now = attend(near, 256 * chunk, 256)
        exp_sums = sums_now if exp_sums is None else [a + b for a, b in zip(exp_sums, sums_now)]

    for head in range(HEADS):
        inverse = 1.0 / exp_sums[head]
        part = slice(HEAD_DIM * head, HEAD_DIM * head + HEAD_DIM)

        probs[head] = (exps[head] * inverse).astype(BF16) * counts_16[...]
        attended[part, :] = dot(values[part, :], probs[head]).astype(BF16)

    mesh_out[...] = (mesh_in[...] + dot(out_t[...], attended[...])).astype(BF16)
    for index, piece in enumerate(pieces_of(dot(dec_t[:ROWS, :], mesh_out[...]), 2)):
        vars_two[ROWS * index : ROWS * index + ROWS, :] = piece
    for flight in target_flights:
        flight.wait_recv()

    scale_all = 1.0 / (MEMBERS * VARS)
    grad_scale = 2.0 * out_scale * scale_all
    grad_net[VARS:, :] = jnp.zeros((ROWS - VARS, 3 * G_DEV), BF16)
    loss_row = jnp.zeros((1, 512), F32)
    sources = ((noisy_ref, target_ref), (state_in.at[0], target_in.at[0]), (state_in.at[1], target_in.at[1]))
    for place, (state, target) in enumerate(sources):
        for chunk in range(4):
            cells = slice(512 * chunk, 512 * chunk + 512)
            block = slice(G_DEV * place + 512 * chunk, G_DEV * place + 512 * chunk + 512)
            both = dot(vars_two[...], table[:, block])
            net = both[:VARS, :] + both[ROWS : ROWS + VARS, :]
            weights = weights_ref[:, block]
            errors = skip_scale * state[:, cells].astype(F32) + out_scale * net - target[:, cells].astype(F32)
            weighted = weights * errors
            loss_row = loss_row + jnp.sum(weighted * errors, axis=0, keepdims=True)
            grad_net[:VARS, block] = (grad_scale * weights * errors).astype(BF16)
    loss = jnp.sum(loss_row, axis=1, keepdims=True) * scale_all
    node_grad = dot_t(grad_net[...], table[...])
    node_pieces = pieces_of(node_grad, 3)
    grown = None
    for piece in node_pieces:
        term = dot(dec_full[:, :ROWS], piece)
        grown = term if grown is None else grown + term
    mesh_grad[...] = grown.astype(BF16)
    head_grad[...] = dot(out_w_ref[...], mesh_grad[...]).astype(BF16)

    units = []
    for index, unit in enumerate(UNITS):
        units.append(
            device_sum(parts[unit[0]], totals[unit[3]], unit, unit_refs[7 * index : 7 * index + 7], copies, at)
        )
    out_units, value_units = (units[:4], units[4:])
    out_sum = dot_t(attended[...], mesh_grad[...])
    for lane in range(4):
        part_out[512 * lane : 512 * lane + 512, :] = out_sum[:, 128 * lane : 128 * lane + 128]
    for unit in out_units[:3]:
        next(unit)
    dec_sum = None
    for piece in node_pieces:
        term = dot_t(piece, mesh_out[...])
        dec_sum = term if dec_sum is None else dec_sum + term
    for lane in range(4):
        part_dec[ROWS * lane : ROWS * lane + ROWS, :] = dec_sum[:, 128 * lane : 128 * lane + 128]
    part_dec[4 * ROWS :, :] = jnp.broadcast_to(loss, (128, 128))
    next(out_units[3])
    def advance(some):
        for unit in some:
            next(unit)

    for head in range(HEADS):
        part = slice(HEAD_DIM * head, HEAD_DIM * head + HEAD_DIM)
        spread = dot_t(head_grad[part, :], probs[head]).astype(BF16)
        part_value[512 * head : 512 * head + 512, :] = dot_t(normed[...], spread[:, :M_DEV]) + dot_t(
            normed_in[...], spread[:, M_DEV:]
        )
        if head == 1:
            advance(out_units)
        if head >= 1:
            next(value_units[head - 1])
        if head >= 2:
            next(value_units[head - 2])
    order = ((value_units[2:],),) + ((out_units, value_units),) * 6
    for groups in order:
        for group in groups:
            advance(group)
    assert [next(unit, "end") for unit in units] == ["end"] * len(units)
    for copy in copies.all:
        copy.wait_send()


def finish_kernel(
    out_a, out_b, value_a, value_b, dec_ref, out_hbm, value_hbm, dec_result, loss_result, sems
):
    flights = []
    for index, (source, tail, target) in enumerate(((out_a, out_b, out_hbm), (value_a, value_b, value_hbm))):
        for lane in range(4):
            flights.append(
                pltpu.make_async_copy(
                    source.at[pl.ds(512 * lane, 512), :] if lane < 3 else tail,
                    target.at[:, pl.ds(128 * lane, 128)],
                    sems.at[4 * index + lane],
                )
            )
            flights[-1].start()
    for lane in range(4):
        dec_result[:, 128 * lane : 128 * lane + 128] = dec_ref[ROWS * lane : ROWS * lane + VARS, :]
    loss_result[...] = dec_ref[4 * ROWS : 4 * ROWS + 1, :1] / GRID
    for flight in flights:
        flight.wait()


def local(
    noisy_state,
    target_state,
    noise_level,
    var_weight,
    embed_in,
    embed_out,
    norm_gain,
    qkv_weight,
    head_scale,
    out_weight,
    dec_weight,
    g2m_node,
    m2g_node,
    neighbours,
):
    vmem = pl.BlockSpec(memory_space=pltpu.VMEM)
    smem = pl.BlockSpec(memory_space=pltpu.SMEM)
    anywhere = pl.BlockSpec(memory_space=pl.ANY)
    copies = 15 + 7 * len(UNITS)
    scratch = [pltpu.SemaphoreType.DMA((copies,))] * 2 + [pltpu.SemaphoreType.DMA((len(INPUTS),))]
    scratch += [pltpu.VMEM(entry[-2], entry[-1]) for entry in INPUTS + SCRATCH]
    for unit in UNITS:
        scratch += sum_scratch(unit[2])
    totals = pl.pallas_call(
        step_kernel,
        out_shape=[pltpu.VMEM(shape, F32) for shape in TOTALS],
        in_specs=[smem] + [anywhere] * len(INPUTS),
        out_specs=[vmem] * len(TOTALS),
        scratch_shapes=scratch,
        compiler_params=pltpu.CompilerParams(
            collective_id=0, has_side_effects=True, vmem_limit_bytes=STEP_VMEM
        ),
        name="step",
    )(
        head_scale,
        noisy_state,
        g2m_node.reshape(1, G_DEV),
        embed_in,
        embed_out,
        norm_gain.reshape(1, D),
        qkv_weight,
        neighbours.T,
        m2g_node.reshape(1, G_DEV),
        out_weight,
        dec_weight.T,
        target_state,
        var_weight.reshape(1, VARS),
        noise_level.reshape(1, 1),
    )
    square = jax.ShapeDtypeStruct((D, D), F32)
    grad_out, grad_value, dec, loss = pl.pallas_call(
        finish_kernel,
        out_shape=(square, square, jax.ShapeDtypeStruct((VARS, D), F32), jax.ShapeDtypeStruct((1, 1), F32)),
        in_specs=[vmem] * len(TOTALS),
        out_specs=(anywhere, anywhere, vmem, vmem),
        scratch_shapes=[pltpu.SemaphoreType.DMA((8,))],
        compiler_params=pltpu.CompilerParams(vmem_limit_bytes=8 << 20),
        name="finish",
    )(*[total.reshape(-1, 128) for total in totals])
    return loss.reshape(()), dec.T, grad_out, grad_value


def solution(mesh):
    in_specs = (
        P(("chan", "member"), None, "band"),
        P(("chan", "member"), None, "band"),
        P(("chan", "member")),
        P(),
        P(),
        P(),
        P(),
        P(),
        P(),
        P(),
        P(),
        P("band"),
        P("band"),
        P("band", None),
    )
    out_specs = (P(), P(), P(), P())
    return jax.shard_map(local, mesh=mesh, in_specs=in_specs, out_specs=out_specs, check_vma=False)
```

```python
import math

import jax
import jax.numpy as jnp
from jax import lax
from jax.experimental import pallas as pl
from jax.experimental.pallas import tpu as pltpu
from jax.sharding import PartitionSpec as P

D = 512
VARS = 84
HEADS = 4
NBR = 32
G_DEV = 2048
M_DEV = 512
HEAD_DIM = 128
GRID = 32768
MEMBERS = 8
WINDOW = 3 * M_DEV
ROWS = 96
BF16, F32, I32 = jnp.bfloat16, jnp.float32, jnp.int32
MESH_ID = pl.DeviceIdType.MESH
UNITS = (
    (0, 0, 768, 0, 0, "xyz"),
    (0, 768, 768, 0, 1, "yzx"),
    (0, 1536, 1024, 1, 0, "zxy"),
    (1, 0, 768, 2, 0, "xyz"),
    (1, 768, 768, 2, 1, "yzx"),
    (1, 1536, 512, 3, 0, "zxy"),
)
TOTALS = ((4, 4, 96, 128), (2, 4, 128, 128), (4, 4, 96, 128), (2, 4, 64, 128))


def coordinates():
    band, chan, core = (lax.axis_index("band"), lax.axis_index("chan"), lax.axis_index("member"))
    return {"band": band, "x": chan, "y": lax.rem(band, 4), "z": band // 4, "core": core}


def peer_on(axis, at, step):
    other = lax.rem(at[axis] + step, 4)
    if axis == "x":
        return (at["band"], other, at["core"])
    if axis == "y":
        return (at["z"] * 4 + other, at["x"], at["core"])
    return (other * 4 + at["y"], at["x"], at["core"])


def sibling(at):
    return (at["band"], at["x"], 1 - at["core"])


class Flight:
    def __init__(self, copies, index, size_ref, device):
        self.index = index
        self.whole = pltpu.make_async_remote_copy(
            src_ref=size_ref,
            dst_ref=size_ref,
            send_sem=copies.send_sems.at[index],
            recv_sem=copies.recv_sems.at[index],
            device_id=device,
            device_id_type=MESH_ID,
        )

    def wait_recv(self):
        self.whole.wait_recv()

    def wait_send(self):
        self.whole.wait_send()


class Copies:
    def __init__(self, send_sems, recv_sems):
        self.send_sems, self.recv_sems, self.all = send_sems, recv_sems, []

    def join(self, flight, group):
        for source, target, device in group:
            pltpu.make_async_remote_copy(
                src_ref=source,
                dst_ref=target,
                send_sem=self.send_sems.at[flight.index],
                recv_sem=self.recv_sems.at[flight.index],
                device_id=device,
                device_id_type=MESH_ID,
            ).start()

    def start(self, size_ref, group):
        index = len(self.all)
        for source, target, device in group:
            pltpu.make_async_remote_copy(
                src_ref=source,
                dst_ref=target,
                send_sem=self.send_sems.at[index],
                recv_sem=self.recv_sems.at[index],
                device_id=device,
                device_id_type=MESH_ID,
            ).start()
        self.all.append(Flight(self, index, size_ref, group[0][2]))
        return self.all[-1]


def greet(devices):
    for device in devices:
        pl.semaphore_signal(
            pltpu.get_barrier_semaphore(), inc=1, device_id=device, device_id_type=MESH_ID
        )


def await_greetings(devices):
    pl.semaphore_wait(pltpu.get_barrier_semaphore(), len(devices))


def sum_partners(at):
    return [sibling(at)] + [peer_on(axis, at, step) for axis in ("x", "y", "z") for step in (1, 2, 3)]


def sum_scratch(rows):
    half = rows // 2
    return [
        pltpu.VMEM((half, 128), F32),
        pltpu.VMEM((half, 128), F32),
        pltpu.VMEM((3, half // 4, 128), F32),
        pltpu.VMEM((half // 4, 128), F32),
        pltpu.VMEM((3, half // 16, 128), F32),
        pltpu.VMEM((4, half // 16, 128), F32),
        pltpu.VMEM((half // 16, 128), F32),
    ]


def device_sum(part, total, unit, refs, copies, at):
    near, pair, first_in, first, second_in, slots, second = refs
    origin, size_all, which, place, (first_axis, second_axis, third_axis) = unit[1:]
    half = size_all // 2
    quarter, tiny = half // 4, half // 16

    def rows(start, size):
        return pl.ds(pl.multiple_of(start, size), size)

    def scatter(source, landing, size, axis):
        group = []
        for step in (1, 2, 3):
            block = source.at[rows(lax.rem(at[axis] + step, 4) * size, size), :]
            group.append((block, landing.at[step - 1], peer_on(axis, at, step)))
        return copies.start(landing, group)

    def gather_sum(source, landing, size, axis, flight):
        flight.wait_recv()
        return (source[rows(at[axis] * size, size), :] + landing[0]) + (landing[1] + landing[2])

    mine = origin + at["core"] * half
    flight = copies.start(
        near, [(part.at[rows(origin + (1 - at["core"]) * half, half), :], near, sibling(at))]
    )
    yield
    flight.wait_recv()
    pair[...] = part[rows(mine, half), :] + near[...]
    flight = scatter(pair, first_in, quarter, first_axis)
    yield
    first[...] = gather_sum(pair, first_in, quarter, first_axis, flight)
    flight = scatter(first, second_in, tiny, second_axis)
    yield
    second[...] = gather_sum(first, second_in, tiny, second_axis, flight)
    slots[at[third_axis]] = second[...]
    flight = copies.start(
        slots.at[pl.ds(0, 3)],
        [(second, slots.at[at[third_axis]], peer_on(third_axis, at, step)) for step in (1, 2, 3)],
    )
    yield
    flight.wait_recv()
    block = 2 * place + at["core"]
    one = total.at[block, at[first_axis], rows(at[second_axis] * tiny, tiny), :]
    total[block, at[first_axis], rows(at[second_axis] * tiny, tiny), :] = (slots[0] + slots[1]) + (
        slots[2] + slots[3]
    )
    flight = copies.start(
        total.at[block, pl.ds(0, 3), rows(0, tiny), :],
        [(one, one, peer_on(first_axis, at, step)) for step in (1, 2, 3)],
    )
    yield
    flight.wait_recv()

    def line_of(place):
        return total.at[block, :, rows(lax.rem(place, 4) * tiny, tiny), :]

    line = line_of(at[second_axis])
    sides = copies.start(
        total.at[block, :, pl.ds(0, 2 * tiny), :],
        [(line, line, peer_on(second_axis, at, step)) for step in (1, 3)],
    )
    across = copies.start(line, [(line, line, peer_on(second_axis, at, 2))])
    flight = copies.start(total.at[block], [(line, line, sibling(at))])
    yield
    sides.wait_recv()
    copies.join(flight, [(line_of(at[second_axis] + step),) * 2 + (sibling(at),) for step in (1, 3)])
    across.wait_recv()
    copies.join(flight, [(line_of(at[second_axis] + 2),) * 2 + (sibling(at),)])
    yield
    flight.wait_recv()
    yield


def dot(left, right):
    return jnp.dot(left, right, preferred_element_type=F32)


def dot_t(left, right):
    return lax.dot_general(left, right, (((1,), (1,)), ((), ())), preferred_element_type=F32)


def pieces_of(values, count):
    pieces, rest = ([], values)
    for index in range(count):
        piece = rest.astype(BF16)
        pieces.append(piece)
        if index + 1 < count:
            rest = rest - piece.astype(F32)
    return pieces


def unit_heads(values, width):
    split = values.reshape(HEADS, HEAD_DIM, width)
    scale = lax.rsqrt(jnp.mean(split * split, axis=1, keepdims=True) + 1e-06)
    return (split * scale).reshape(D, width)


def lanes(values, width):
    return jnp.concatenate([values] * (width // 128), axis=1)


STEP_VMEM = 59 << 20
CHUNKS = ((0, 512), (512, 512), (1024, 512), (1536, 256), (1792, 256))
INPUTS = (
    ("noisy", (VARS, G_DEV), BF16),
    ("g2m", (1, G_DEV), I32),
    ("embed_in", (VARS, D), BF16),
    ("embed_out", (D, D), BF16),
    ("gain", (1, D), F32),
    ("qkv", (3, D, D), BF16),
    ("nbr", (NBR, M_DEV), I32),
    ("m2g", (1, G_DEV), I32),
    ("out_w", (D, D), BF16),
    ("dec_w", (VARS, D), BF16),
    ("target", (VARS, G_DEV), BF16),
    ("var", (1, VARS), F32),
    ("level", (1, 1), F32),
    ("head_scale", (1, HEADS), F32),
)

SCRATCH = (
    ((2, VARS, G_DEV), BF16),
    ((2, VARS, G_DEV), BF16),
    ((2, 1, G_DEV), I32),
    ((2, 1, G_DEV), I32),
    ((128, D), BF16),
    ((D, 128), BF16),
    ((128, D), BF16),
    ((D, 128), BF16),
    ((D, D), BF16),
    ((D, D), BF16),
    ((D, D), BF16),
    ((D, D), BF16),
    ((D, D), BF16),
    ((D, M_DEV), F32),
    ((D, M_DEV), F32),
    ((D, M_DEV), BF16),
    ((D, 2 * M_DEV), BF16),
    ((D, M_DEV), BF16),
    ((WINDOW, D), BF16),
    ((D, WINDOW), BF16),
    ((NBR, M_DEV), I32),
    ((NBR, M_DEV), I32),
    ((WINDOW, M_DEV), F32),
    ((WINDOW, M_DEV), BF16),
    ((HEADS, WINDOW, M_DEV), F32),
    ((HEADS, WINDOW, M_DEV), BF16),
    ((D, M_DEV), BF16),
    ((D, M_DEV), BF16),
    ((M_DEV, 3 * G_DEV), BF16),
    ((2 * ROWS, M_DEV), BF16),
    ((VARS, 3 * G_DEV), F32),
    ((ROWS, 3 * G_DEV), BF16),
    ((D, M_DEV), BF16),
    ((D, M_DEV), BF16),
    ((2560, 128), F32),
    ((2048, 128), F32),
    ((D, 128), F32),
)


def step_kernel(*refs):
    hbm, totals = refs[: len(INPUTS)], refs[len(INPUTS) : len(INPUTS) + len(TOTALS)]
    scratch = refs[len(INPUTS) + len(TOTALS) :]
    send_sems, recv_sems, load_sems = scratch[:3]
    held = dict(zip([name for name, shape, kind in INPUTS], scratch[3:]))
    unit_refs = scratch[3 + len(INPUTS + SCRATCH) :]
    (
        noisy_ref,
        g2m_ref,
        embed_in_ref,
        embed_out_ref,
        gain_ref,
        qkv_ref,
        nbr_ref,
        m2g_ref,
        out_w_ref,
        dec_w_ref,
        target_ref,
        var_ref,
        level_ref,
        head_scale_ref,
    ) = scratch[3 : 3 + len(INPUTS)]
    (
        state_in,
        target_in,
        g2m_in,
        m2g_in,
        pad_in,
        embed_in_t,
        dec_t,
        dec_full,
        embed_out_t,
        q_t,
        k_t,
        v_t,
        out_t,
        node_hidden,
        mesh_in,
        normed,
        normed_in,
        unit_q,
        unit_k,
        values,
        within,
        fields,
        counts,
        counts_16,
        exps,
        probs,
        attended,
        mesh_out,
        table,
        vars_two,
        weights_ref,
        grad_net,
        mesh_grad,
        head_grad,
        part_out,
        part_value,
        gain_t,
    ) = scratch[3 + len(INPUTS) : 3 + len(INPUTS + SCRATCH)]
    parts = (part_out, part_value)
    at = coordinates()
    band = at["band"]
    left = (lax.rem(band + 15, 16), at["x"], at["core"])
    right = (lax.rem(band + 1, 16), at["x"], at["core"])
    sides = ((0, left, 1), (1, right, 0))
    base = band * M_DEV
    copies = Copies(send_sems, recv_sems)
    partners = [left, right] + sum_partners(at)
    greet(partners)
    loads = {}
    for index, (name, shape, kind) in enumerate(INPUTS):
        source = hbm[index].at[0] if name in ("noisy", "target") else hbm[index]
        loads[name] = pltpu.make_async_copy(source, held[name], load_sems.at[index])
        loads[name].start()
    loads["noisy"].wait()
    loads["g2m"].wait()
    await_greetings(partners)

    node_flight = copies.start(g2m_in, [(g2m_ref, g2m_in.at[slot], device) for side, device, slot in sides])
    state_flights = []
    for first, size in CHUNKS:
        cells = pl.ds(first, size)
        state_flights.append(
            copies.start(
                state_in.at[:, :, cells],
                [
                    (noisy_ref.at[:, cells], state_in.at[slot, :, cells], device)
                    for side, device, slot in sides
                ],
            )
        )


    def send_target(first, size):
        cells = pl.ds(first, size)
        return copies.start(
            target_in.at[:, :, cells],
            [(target_ref.at[:, cells], target_in.at[slot, :, cells], device) for side, device, slot in sides],
        )

    loads["m2g"].wait()
    cell_flight = copies.start(m2g_in, [(m2g_ref, m2g_in.at[slot], device) for side, device, slot in sides])
    loads["target"].wait()
    target_flights = [send_target(512 * chunk, 512) for chunk in range(2)]
    loads["embed_in"].wait()
    pad_in[...] = jnp.zeros_like(pad_in)
    pad_in[:VARS, :] = embed_in_ref[...]
    embed_in_t[...] = jnp.transpose(pad_in[...])
    loads["level"].wait()
    level = level_ref[...]
    level_sq = level * level + 1.0
    scale_in = lax.rsqrt(level_sq)
    skip_scale = 1.0 / level_sq
    out_scale = level * scale_in
    half_scale = 0.5 * scale_in

    def encode(state, nodes):
        half_t = dot(embed_in_t[:, :VARS], state) * half_scale
        hidden = (half_t + half_t * jnp.tanh(half_t)).astype(BF16)
        ids = lax.broadcasted_iota(I32, (M_DEV, state.shape[1]), 0)
        chosen = jnp.where(nodes - base == ids, 1.0, 0.0).astype(BF16)
        node_hidden[...] += dot_t(hidden, chosen)

    node_hidden[...] = jnp.zeros_like(node_hidden)

    @pl.loop(0, 4)
    def _(chunk):
        cells = pl.ds(pl.multiple_of(chunk * 512, 512), 512)
        encode(noisy_ref[:, cells], g2m_ref[:, cells])

    loads["embed_out"].wait()
    embed_out_t[...] = jnp.transpose(embed_out_ref[...])
    loads["var"].wait()
    square = lax.broadcasted_iota(I32, (VARS, VARS), 0) == lax.broadcasted_iota(I32, (VARS, VARS), 1)
    var_column = jnp.sum(jnp.where(square, var_ref[...], 0.0), axis=1, keepdims=True)

    def prepare(place, nodes):
        local = nodes - base
        ids = lax.broadcasted_iota(I32, (M_DEV, G_DEV), 0)
        block = slice(G_DEV * place, G_DEV * place + G_DEV)
        table[:, block] = jnp.where(local == ids, 1.0, 0.0).astype(BF16)
        cells = lax.broadcasted_iota(I32, (1, G_DEV), 1) + lax.rem(band + (0, 15, 1)[place], 16) * G_DEV
        lat_weight = 0.2 + jnp.cos(math.pi * (cells.astype(F32) + 0.5) / GRID - 0.5 * math.pi)
        mine = (local >= 0) & (local < M_DEV)
        weights_ref[:, block] = var_column * jnp.where(mine, lat_weight, 0.0)

    prepare(0, m2g_ref[...])
    loads["gain"].wait()
    gain_t[...] = jnp.transpose(jnp.broadcast_to(gain_ref[...], (128, D)))
    node_flight.wait_recv()
    for (first, size), flight in zip(CHUNKS, state_flights):
        cells = slice(first, first + size)
        flight.wait_recv()

        for slot in range(2):
            encode(state_in[slot, :, cells], g2m_in[slot, :, cells])

    encoded = None
    for piece in pieces_of(node_hidden[...], 2):
        term = dot(embed_out_t[...], piece)
        encoded = term if encoded is None else encoded + term
    mesh_in[...] = encoded
    mean_sq = jnp.mean(encoded * encoded, axis=0, keepdims=True)
    gain = lanes(gain_t[...], M_DEV)
    normed[...] = (encoded * lax.rsqrt(mean_sq + 1e-05) * gain).astype(BF16)

    normed_flights = []
    for chunk in range(4):
        nodes = pl.ds(128 * chunk, 128)
        normed_flights.append(
            copies.start(
                normed_in.at[:, pl.ds(256 * chunk, 256)],
                [
                    (normed.at[:, nodes], normed_in.at[:, pl.ds(256 * chunk + 128 * slot, 128)], device)
                    for side, device, slot in sides
                ],
            )
        )

    target_flights += [send_target(512 * chunk, 512) for chunk in range(2, 4)]

    loads["qkv"].wait()
    q_t[...] = jnp.transpose(qkv_ref[0])
    k_t[...] = jnp.transpose(qkv_ref[1])
    v_t[...] = jnp.transpose(qkv_ref[2])
    unit_q[...] = unit_heads(dot(q_t[...], normed[...]), M_DEV).astype(BF16)

    loads["head_scale"].wait()
    score_scale = head_scale_ref[...] / HEAD_DIM

    def attend(near, start, width):
        keys = unit_heads(dot(k_t[...], near), width).astype(BF16)
        unit_k[start : start + width, :] = jnp.transpose(keys)
        values[:, start : start + width] = dot(v_t[...], near).astype(BF16)
        sums_now = []
        count = counts[start : start + width, :]
        for head in range(HEADS):
            part = slice(HEAD_DIM * head, HEAD_DIM * head + HEAD_DIM)
            scores = dot(unit_k[start : start + width, part], unit_q[part, :])
            exp = jnp.exp(scores * score_scale[:, head : head + 1])
            exps[head, start : start + width, :] = exp
            sums_now.append(jnp.sum(exp * count, axis=0, keepdims=True))
        return sums_now

    loads["nbr"].wait()
    window = nbr_ref[...] - (base - M_DEV)
    patch = lax.shift_right_arithmetic(window, jnp.full_like(window, 9))
    within[...] = window - patch * M_DEV
    fields[...] = jnp.where(patch == 0, 64, jnp.where(patch == 1, 1, 4096))

    @pl.loop(0, 8)
    def _(block):
        ids = lax.broadcasted_iota(I32, (64, M_DEV), 0) + block * 64
        total = jnp.zeros((64, M_DEV), I32)
        for j in range(NBR):
            total = total + jnp.where(within[j : j + 1, :] == ids, fields[j : j + 1, :], 0)
        chunk = block // 2
        part = (block - 2 * chunk) * 64
        for start, shift in (
            (block * 64, 0),
            (M_DEV + 256 * chunk + part, 6),
            (M_DEV + 256 * chunk + 128 + part, 12),
        ):
            count = lax.shift_right_logical(total, jnp.full_like(total, shift)) & 63
            rows = pl.ds(pl.multiple_of(start, 64), 64)
            counts[rows, :] = count.astype(F32)
            counts_16[rows, :] = count.astype(F32).astype(BF16)

    cell_flight.wait_recv()
    for slot in range(2):
        prepare(1 + slot, m2g_in[slot])

    loads["out_w"].wait()
    loads["dec_w"].wait()
    out_t[...] = jnp.transpose(out_w_ref[...])
    dec_t[...] = jnp.zeros_like(dec_t)
    dec_t[:VARS, :] = dec_w_ref[...]
    dec_full[...] = jnp.transpose(dec_t[...])
    exp_sums = None
    for chunk in range(6):
        if chunk < 2:
            near = normed[:, 256 * chunk : 256 * chunk + 256]
        else:
            normed_flights[chunk - 2].wait_recv()
            near = normed_in[:, 256 * (chunk - 2) : 256 * (chunk - 2) + 256]
        sums_now = attend(near, 256 * chunk, 256)
        exp_sums = sums_now if exp_sums is None else [a + b for a, b in zip(exp_sums, sums_now)]

    for head in range(HEADS):
        inverse = 1.0 / exp_sums[head]
        part = slice(HEAD_DIM * head, HEAD_DIM * head + HEAD_DIM)

        probs[head] = (exps[head] * inverse).astype(BF16) * counts_16[...]
        attended[part, :] = dot(values[part, :], probs[head]).astype(BF16)

    mesh_out[...] = (mesh_in[...] + dot(out_t[...], attended[...])).astype(BF16)
    for index, piece in enumerate(pieces_of(dot(dec_t[:ROWS, :], mesh_out[...]), 2)):
        vars_two[ROWS * index : ROWS * index + ROWS, :] = piece
    scale_all = 1.0 / (MEMBERS * VARS)
    grad_scale = 2.0 * out_scale * scale_all
    grad_net[VARS:, :] = jnp.zeros((ROWS - VARS, 3 * G_DEV), BF16)
    loss_row = jnp.zeros((1, 512), F32)
    sources = ((noisy_ref, target_ref), (state_in.at[0], target_in.at[0]), (state_in.at[1], target_in.at[1]))
    chunks = [(0, chunk) for chunk in range(4)] + [(place, chunk) for chunk in range(4) for place in (1, 2)]
    for place, chunk in chunks:
        state, target = sources[place]
        if place == 1 and chunk == 0:
            target_flights[0].wait_recv()
            target_flights[1].wait_recv()
        if place == 1 and chunk == 2:
            target_flights[2].wait_recv()
            target_flights[3].wait_recv()
        cells = slice(512 * chunk, 512 * chunk + 512)
        block = slice(G_DEV * place + 512 * chunk, G_DEV * place + 512 * chunk + 512)
        both = dot(vars_two[...], table[:, block])
        net = both[:VARS, :] + both[ROWS : ROWS + VARS, :]
        weights = weights_ref[:, block]
        errors = skip_scale * state[:, cells].astype(F32) + out_scale * net - target[:, cells].astype(F32)
        weighted = weights * errors
        loss_row = loss_row + jnp.sum(weighted * errors, axis=0, keepdims=True)
        grad_net[:VARS, block] = (grad_scale * weights * errors).astype(BF16)
    loss = jnp.sum(loss_row, axis=1, keepdims=True) * scale_all
    node_grad = dot_t(grad_net[...], table[...])
    node_pieces = pieces_of(node_grad, 2)
    grown = None
    for piece in node_pieces:
        term = dot(dec_full[:, :ROWS], piece)
        grown = term if grown is None else grown + term
    mesh_grad[...] = grown.astype(BF16)
    head_grad[...] = dot(out_w_ref[...], mesh_grad[...]).astype(BF16)

    units = []
    for index, unit in enumerate(UNITS):
        units.append(
            device_sum(parts[unit[0]], totals[unit[3]], unit, unit_refs[7 * index : 7 * index + 7], copies, at)
        )
    out_units, value_units = (units[:3], units[3:])
    out_sum = dot_t(attended[...], mesh_grad[...])
    for lane in range(4):
        part_out[512 * lane : 512 * lane + 512, :] = out_sum[:, 128 * lane : 128 * lane + 128]
    for unit in out_units[:2]:
        next(unit)
    dec_sum = None
    for piece in node_pieces:
        term = dot_t(piece, mesh_out[...])
        dec_sum = term if dec_sum is None else dec_sum + term
    for lane in range(4):
        start = 2048 + ROWS * lane
        part_out[start : start + ROWS, :] = dec_sum[:, 128 * lane : 128 * lane + 128]
    part_out[2048 + 4 * ROWS :, :] = jnp.broadcast_to(loss, (128, 128))
    next(out_units[2])
    def advance(some):
        for unit in some:
            next(unit)

    for pair in range(2):
        spread = jnp.concatenate(
            [
                dot_t(head_grad[HEAD_DIM * head : HEAD_DIM * head + HEAD_DIM, :], probs[head]).astype(BF16)
                for head in (2 * pair, 2 * pair + 1)
            ],
            axis=0,
        )
        both = dot_t(normed[...], spread[:, :M_DEV]) + dot_t(normed_in[...], spread[:, M_DEV:])
        for index in range(2):
            start = 1024 * pair + 512 * index
            part_value[start : start + 512, :] = both[:, HEAD_DIM * index : HEAD_DIM * index + HEAD_DIM]
        if pair == 0:
            next(value_units[0])
            advance(out_units)
    advance(value_units[1:])
    next(value_units[0])
    order = ((value_units[1:],),) + ((out_units, value_units),) * 6
    for groups in order:
        for group in groups:
            advance(group)
    assert [next(unit, "end") for unit in units] == ["end"] * len(units)
    for copy in copies.all:
        copy.wait_send()


def finish_kernel(out_a, out_b, value_a, value_b, out_hbm, value_hbm, dec_result, loss_result, sems):
    flights = []
    for index, (source, tail, target) in enumerate(((out_a, out_b, out_hbm), (value_a, value_b, value_hbm))):
        for lane in range(4):
            flights.append(
                pltpu.make_async_copy(
                    source.at[pl.ds(512 * lane, 512), :] if lane < 3 else tail.at[pl.ds(0, 512), :],
                    target.at[:, pl.ds(128 * lane, 128)],
                    sems.at[4 * index + lane],
                )
            )
            flights[-1].start()
    for lane in range(4):
        start = 512 + ROWS * lane
        dec_result[:, 128 * lane : 128 * lane + 128] = out_b[start : start + VARS, :]
    loss_result[...] = out_b[512 + 4 * ROWS : 513 + 4 * ROWS, :1] / GRID
    for flight in flights:
        flight.wait()


def local(
    noisy_state,
    target_state,
    noise_level,
    var_weight,
    embed_in,
    embed_out,
    norm_gain,
    qkv_weight,
    head_scale,
    out_weight,
    dec_weight,
    g2m_node,
    m2g_node,
    neighbours,
):
    vmem = pl.BlockSpec(memory_space=pltpu.VMEM)
    anywhere = pl.BlockSpec(memory_space=pl.ANY)
    copies = 15 + 8 * len(UNITS)
    scratch = [pltpu.SemaphoreType.DMA((copies,))] * 2 + [pltpu.SemaphoreType.DMA((len(INPUTS),))]
    scratch += [pltpu.VMEM(entry[-2], entry[-1]) for entry in INPUTS + SCRATCH]
    for unit in UNITS:
        scratch += sum_scratch(unit[2])
    totals = pl.pallas_call(
        step_kernel,
        out_shape=[pltpu.VMEM(shape, F32) for shape in TOTALS],
        in_specs=[anywhere] * len(INPUTS),
        out_specs=[vmem] * len(TOTALS),
        scratch_shapes=scratch,
        compiler_params=pltpu.CompilerParams(
            collective_id=0, has_side_effects=True, vmem_limit_bytes=STEP_VMEM
        ),
        name="step",
    )(
        noisy_state,
        g2m_node.reshape(1, G_DEV),
        embed_in,
        embed_out,
        norm_gain.reshape(1, D),
        qkv_weight,
        neighbours.T,
        m2g_node.reshape(1, G_DEV),
        out_weight,
        dec_weight.T,
        target_state,
        var_weight.reshape(1, VARS),
        noise_level.reshape(1, 1),
        head_scale.reshape(1, HEADS),
    )
    square = jax.ShapeDtypeStruct((D, D), F32)
    grad_out, grad_value, dec, loss = pl.pallas_call(
        finish_kernel,
        out_shape=(square, square, jax.ShapeDtypeStruct((VARS, D), F32), jax.ShapeDtypeStruct((1, 1), F32)),
        in_specs=[vmem] * len(TOTALS),
        out_specs=(anywhere, anywhere, vmem, vmem),
        scratch_shapes=[pltpu.SemaphoreType.DMA((8,))],
        compiler_params=pltpu.CompilerParams(vmem_limit_bytes=8 << 20),
        name="finish",
    )(*[total.reshape(-1, 128) for total in totals])
    return loss.reshape(()), dec.T, grad_out, grad_value


def solution(mesh):
    in_specs = (
        P(("chan", "member"), None, "band"),
        P(("chan", "member"), None, "band"),
        P(("chan", "member")),
        P(),
        P(),
        P(),
        P(),
        P(),
        P(),
        P(),
        P(),
        P("band"),
        P("band"),
        P("band", None),
    )
    out_specs = (P(), P(), P(), P())
    return jax.shard_map(local, mesh=mesh, in_specs=in_specs, out_specs=out_specs, check_vma=False)
```

```python
import math

import jax
import jax.numpy as jnp
from jax import lax
from jax.experimental import pallas as pl
from jax.experimental.pallas import tpu as pltpu
from jax.sharding import PartitionSpec as P

D = 512
VARS = 84
HEADS = 4
NBR = 32
G_DEV = 2048
M_DEV = 512
HEAD_DIM = 128
GRID = 32768
MEMBERS = 8
WINDOW = 3 * M_DEV
ROWS = 96
BF16, F32, I32 = jnp.bfloat16, jnp.float32, jnp.int32
MESH_ID = pl.DeviceIdType.MESH
UNITS = (
    (0, 0, 768, 0, 0, "xyz"),
    (0, 768, 768, 0, 1, "yzx"),
    (0, 1536, 1024, 1, 0, "zxy"),
    (1, 0, 768, 2, 0, "xyz"),
    (1, 768, 768, 2, 1, "yzx"),
    (1, 1536, 512, 3, 0, "zxy"),
)
TOTALS = ((4, 4, 96, 128), (2, 4, 128, 128), (4, 4, 96, 128), (2, 4, 64, 128))


def coordinates():
    band, chan, core = (lax.axis_index("band"), lax.axis_index("chan"), lax.axis_index("member"))
    return {"band": band, "x": chan, "y": lax.rem(band, 4), "z": band // 4, "core": core}


def peer_on(axis, at, step):
    other = lax.rem(at[axis] + step, 4)
    if axis == "x":
        return (at["band"], other, at["core"])
    if axis == "y":
        return (at["z"] * 4 + other, at["x"], at["core"])
    return (other * 4 + at["y"], at["x"], at["core"])


def sibling(at):
    return (at["band"], at["x"], 1 - at["core"])


class Flight:
    def __init__(self, copies, index, size_ref, device):
        self.index = index
        self.whole = pltpu.make_async_remote_copy(
            src_ref=size_ref,
            dst_ref=size_ref,
            send_sem=copies.send_sems.at[index],
            recv_sem=copies.recv_sems.at[index],
            device_id=device,
            device_id_type=MESH_ID,
        )

    def wait_recv(self):
        self.whole.wait_recv()

    def wait_send(self):
        self.whole.wait_send()


class Copies:
    def __init__(self, send_sems, recv_sems):
        self.send_sems, self.recv_sems, self.all = send_sems, recv_sems, []

    def join(self, flight, group):
        for source, target, device in group:
            pltpu.make_async_remote_copy(
                src_ref=source,
                dst_ref=target,
                send_sem=self.send_sems.at[flight.index],
                recv_sem=self.recv_sems.at[flight.index],
                device_id=device,
                device_id_type=MESH_ID,
            ).start()

    def start(self, size_ref, group):
        index = len(self.all)
        for source, target, device in group:
            pltpu.make_async_remote_copy(
                src_ref=source,
                dst_ref=target,
                send_sem=self.send_sems.at[index],
                recv_sem=self.recv_sems.at[index],
                device_id=device,
                device_id_type=MESH_ID,
            ).start()
        self.all.append(Flight(self, index, size_ref, group[0][2]))
        return self.all[-1]


def greet(devices):
    for device in devices:
        pl.semaphore_signal(
            pltpu.get_barrier_semaphore(), inc=1, device_id=device, device_id_type=MESH_ID
        )


def await_greetings(devices):
    pl.semaphore_wait(pltpu.get_barrier_semaphore(), len(devices))


def sum_partners(at):
    return [sibling(at)] + [peer_on(axis, at, step) for axis in ("x", "y", "z") for step in (1, 2, 3)]


def sum_scratch(rows):
    half = rows // 2
    return [
        pltpu.VMEM((half, 128), F32),
        pltpu.VMEM((half, 128), F32),
        pltpu.VMEM((3, half // 4, 128), F32),
        pltpu.VMEM((half // 4, 128), F32),
        pltpu.VMEM((3, half // 16, 128), F32),
        pltpu.VMEM((4, half // 16, 128), F32),
        pltpu.VMEM((half // 16, 128), F32),
    ]


def device_sum(part, total, unit, refs, copies, at):
    near, pair, first_in, first, second_in, slots, second = refs
    origin, size_all, which, place, (first_axis, second_axis, third_axis) = unit[1:]
    half = size_all // 2
    quarter, tiny = half // 4, half // 16

    def rows(start, size):
        return pl.ds(pl.multiple_of(start, size), size)

    def scatter(source, landing, size, axis):
        group = []
        for step in (1, 2, 3):
            block = source.at[rows(lax.rem(at[axis] + step, 4) * size, size), :]
            group.append((block, landing.at[step - 1], peer_on(axis, at, step)))
        return copies.start(landing, group)

    def gather_sum(source, landing, size, axis, flight):
        flight.wait_recv()
        return (source[rows(at[axis] * size, size), :] + landing[0]) + (landing[1] + landing[2])

    mine = origin + at["core"] * half
    flight = copies.start(
        near, [(part.at[rows(origin + (1 - at["core"]) * half, half), :], near, sibling(at))]
    )
    yield
    flight.wait_recv()
    pair[...] = part[rows(mine, half), :] + near[...]
    flight = scatter(pair, first_in, quarter, first_axis)
    yield
    first[...] = gather_sum(pair, first_in, quarter, first_axis, flight)
    flight = scatter(first, second_in, tiny, second_axis)
    yield
    second[...] = gather_sum(first, second_in, tiny, second_axis, flight)
    slots[at[third_axis]] = second[...]
    flight = copies.start(
        slots.at[pl.ds(0, 3)],
        [(second, slots.at[at[third_axis]], peer_on(third_axis, at, step)) for step in (1, 2, 3)],
    )
    yield
    flight.wait_recv()
    block = 2 * place + at["core"]
    one = total.at[block, at[first_axis], rows(at[second_axis] * tiny, tiny), :]
    total[block, at[first_axis], rows(at[second_axis] * tiny, tiny), :] = (slots[0] + slots[1]) + (
        slots[2] + slots[3]
    )
    flight = copies.start(
        total.at[block, pl.ds(0, 3), rows(0, tiny), :],
        [(one, one, peer_on(first_axis, at, step)) for step in (1, 2, 3)],
    )
    yield
    flight.wait_recv()

    def line_of(place):
        return total.at[block, :, rows(lax.rem(place, 4) * tiny, tiny), :]

    line = line_of(at[second_axis])
    sides = copies.start(
        total.at[block, :, pl.ds(0, 2 * tiny), :],
        [(line, line, peer_on(second_axis, at, step)) for step in (1, 3)],
    )
    across = copies.start(line, [(line, line, peer_on(second_axis, at, 2))])
    flight = copies.start(total.at[block], [(line, line, sibling(at))])
    yield
    sides.wait_recv()
    copies.join(flight, [(line_of(at[second_axis] + step),) * 2 + (sibling(at),) for step in (1, 3)])
    across.wait_recv()
    copies.join(flight, [(line_of(at[second_axis] + 2),) * 2 + (sibling(at),)])
    yield
    flight.wait_recv()
    yield


def dot(left, right):
    return jnp.dot(left, right, preferred_element_type=F32)


def dot_t(left, right):
    return lax.dot_general(left, right, (((1,), (1,)), ((), ())), preferred_element_type=F32)


def pieces_of(values, count):
    pieces, rest = ([], values)
    for index in range(count):
        piece = rest.astype(BF16)
        pieces.append(piece)
        if index + 1 < count:
            rest = rest - piece.astype(F32)
    return pieces


def unit_heads(values, width):
    split = values.reshape(HEADS, HEAD_DIM, width)
    scale = lax.rsqrt(jnp.mean(split * split, axis=1, keepdims=True) + 1e-06)
    return (split * scale).reshape(D, width)


def lanes(values, width):
    return jnp.concatenate([values] * (width // 128), axis=1)


STEP_VMEM = 61 << 20
CHUNKS = ((0, 512), (512, 512), (1024, 512), (1536, 256), (1792, 256))
INPUTS = (
    ("noisy", (VARS, G_DEV), BF16),
    ("g2m", (1, G_DEV), I32),
    ("embed_in", (VARS, D), BF16),
    ("embed_out", (D, D), BF16),
    ("gain", (1, D), F32),
    ("qkv", (3, D, D), BF16),
    ("nbr", (NBR, M_DEV), I32),
    ("m2g", (1, G_DEV), I32),
    ("out_w", (D, D), BF16),
    ("dec_w", (VARS, D), BF16),
    ("target", (VARS, G_DEV), BF16),
    ("var", (1, VARS), F32),
    ("level", (1, 1), F32),
    ("head_scale", (1, HEADS), F32),
)

SCRATCH = (
    ((2, VARS, G_DEV), BF16),
    ((2, VARS, G_DEV), BF16),
    ((2, 1, G_DEV), I32),
    ((2, 1, G_DEV), I32),
    ((128, D), BF16),
    ((D, 128), BF16),
    ((128, D), BF16),
    ((D, 128), BF16),
    ((D, D), BF16),
    ((D, D), BF16),
    ((D, D), BF16),
    ((D, D), BF16),
    ((D, D), BF16),
    ((D, M_DEV), F32),
    ((D, M_DEV), F32),
    ((D, M_DEV), BF16),
    ((D, 2 * M_DEV), BF16),
    ((D, M_DEV), BF16),
    ((WINDOW, D), BF16),
    ((D, WINDOW), BF16),
    ((NBR, M_DEV), I32),
    ((NBR, M_DEV), I32),
    ((WINDOW, M_DEV), F32),
    ((WINDOW, M_DEV), BF16),
    ((HEADS, WINDOW, M_DEV), F32),
    ((HEADS, WINDOW, M_DEV), BF16),
    ((D, M_DEV), BF16),
    ((D, M_DEV), BF16),
    ((M_DEV, 3 * G_DEV), BF16),
    ((2 * ROWS, M_DEV), BF16),
    ((VARS, 3 * G_DEV), F32),
    ((ROWS, 3 * G_DEV), BF16),
    ((D, M_DEV), BF16),
    ((D, M_DEV), BF16),
    ((2560, 128), F32),
    ((2048, 128), F32),
    ((D, 128), F32),
    ((3 * G_DEV, M_DEV), BF16),
)


def step_kernel(*refs):
    hbm, totals = refs[: len(INPUTS)], refs[len(INPUTS) : len(INPUTS) + len(TOTALS)]
    scratch = refs[len(INPUTS) + len(TOTALS) :]
    send_sems, recv_sems, load_sems = scratch[:3]
    held = dict(zip([name for name, shape, kind in INPUTS], scratch[3:]))
    unit_refs = scratch[3 + len(INPUTS + SCRATCH) :]
    (
        noisy_ref,
        g2m_ref,
        embed_in_ref,
        embed_out_ref,
        gain_ref,
        qkv_ref,
        nbr_ref,
        m2g_ref,
        out_w_ref,
        dec_w_ref,
        target_ref,
        var_ref,
        level_ref,
        head_scale_ref,
    ) = scratch[3 : 3 + len(INPUTS)]
    (
        state_in,
        target_in,
        g2m_in,
        m2g_in,
        pad_in,
        embed_in_t,
        dec_t,
        dec_full,
        embed_out_t,
        q_t,
        k_t,
        v_t,
        out_t,
        node_hidden,
        mesh_in,
        normed,
        normed_in,
        unit_q,
        unit_k,
        values,
        within,
        fields,
        counts,
        counts_16,
        exps,
        probs,
        attended,
        mesh_out,
        table,
        vars_two,
        weights_ref,
        grad_net,
        mesh_grad,
        head_grad,
        part_out,
        part_value,
        gain_t,
        table_t,
    ) = scratch[3 + len(INPUTS) : 3 + len(INPUTS + SCRATCH)]
    parts = (part_out, part_value)
    at = coordinates()
    band = at["band"]
    left = (lax.rem(band + 15, 16), at["x"], at["core"])
    right = (lax.rem(band + 1, 16), at["x"], at["core"])
    sides = ((0, left, 1), (1, right, 0))
    base = band * M_DEV
    copies = Copies(send_sems, recv_sems)
    partners = [left, right] + sum_partners(at)
    greet(partners)
    loads = {}
    for index, (name, shape, kind) in enumerate(INPUTS):
        source = hbm[index].at[0] if name in ("noisy", "target") else hbm[index]
        loads[name] = pltpu.make_async_copy(source, held[name], load_sems.at[index])
        loads[name].start()
    loads["noisy"].wait()
    loads["g2m"].wait()
    await_greetings(partners)

    node_flight = copies.start(g2m_in, [(g2m_ref, g2m_in.at[slot], device) for side, device, slot in sides])
    state_flights = []
    for first, size in CHUNKS:
        cells = pl.ds(first, size)
        state_flights.append(
            copies.start(
                state_in.at[:, :, cells],
                [
                    (noisy_ref.at[:, cells], state_in.at[slot, :, cells], device)
                    for side, device, slot in sides
                ],
            )
        )


    def send_target(first, size):
        cells = pl.ds(first, size)
        return copies.start(
            target_in.at[:, :, cells],
            [(target_ref.at[:, cells], target_in.at[slot, :, cells], device) for side, device, slot in sides],
        )

    loads["m2g"].wait()
    cell_flight = copies.start(m2g_in, [(m2g_ref, m2g_in.at[slot], device) for side, device, slot in sides])
    loads["target"].wait()
    target_flights = [send_target(512 * chunk, 512) for chunk in range(2)]
    loads["embed_in"].wait()
    pad_in[...] = jnp.zeros_like(pad_in)
    pad_in[:VARS, :] = embed_in_ref[...]
    embed_in_t[...] = jnp.transpose(pad_in[...])
    loads["level"].wait()
    level = level_ref[...]
    level_sq = level * level + 1.0
    scale_in = lax.rsqrt(level_sq)
    skip_scale = 1.0 / level_sq
    out_scale = level * scale_in
    half_scale = 0.5 * scale_in

    def encode(state, nodes):
        half_t = dot(embed_in_t[:, :VARS], state) * half_scale
        hidden = (half_t + half_t * jnp.tanh(half_t)).astype(BF16)
        ids = lax.broadcasted_iota(I32, (M_DEV, state.shape[1]), 0)
        chosen = jnp.where(nodes - base == ids, 1.0, 0.0).astype(BF16)
        node_hidden[...] += dot_t(hidden, chosen)

    node_hidden[...] = jnp.zeros_like(node_hidden)

    @pl.loop(0, 4)
    def _(chunk):
        cells = pl.ds(pl.multiple_of(chunk * 512, 512), 512)
        encode(noisy_ref[:, cells], g2m_ref[:, cells])

    loads["embed_out"].wait()
    embed_out_t[...] = jnp.transpose(embed_out_ref[...])
    loads["var"].wait()
    square = lax.broadcasted_iota(I32, (VARS, VARS), 0) == lax.broadcasted_iota(I32, (VARS, VARS), 1)
    var_column = jnp.sum(jnp.where(square, var_ref[...], 0.0), axis=1, keepdims=True)

    def prepare(place, nodes):
        local = nodes - base
        ids = lax.broadcasted_iota(I32, (M_DEV, G_DEV), 0)
        block = slice(G_DEV * place, G_DEV * place + G_DEV)
        table[:, block] = jnp.where(local == ids, 1.0, 0.0).astype(BF16)
        upright = jnp.transpose(jnp.broadcast_to(local.astype(F32), (128, G_DEV))).astype(I32)
        for lane in range(4):
            ids = lax.broadcasted_iota(I32, (G_DEV, 128), 1) + 128 * lane
            table_t[block, 128 * lane : 128 * lane + 128] = jnp.where(upright == ids, 1.0, 0.0).astype(BF16)
        cells = lax.broadcasted_iota(I32, (1, G_DEV), 1) + lax.rem(band + (0, 15, 1)[place], 16) * G_DEV
        lat_weight = 0.2 + jnp.cos(math.pi * (cells.astype(F32) + 0.5) / GRID - 0.5 * math.pi)
        mine = (local >= 0) & (local < M_DEV)
        weights_ref[:, block] = var_column * jnp.where(mine, lat_weight, 0.0)

    prepare(0, m2g_ref[...])
    loads["gain"].wait()
    gain_t[...] = jnp.transpose(jnp.broadcast_to(gain_ref[...], (128, D)))
    node_flight.wait_recv()
    for (first, size), flight in zip(CHUNKS, state_flights):
        cells = slice(first, first + size)
        flight.wait_recv()

        for slot in range(2):
            encode(state_in[slot, :, cells], g2m_in[slot, :, cells])

    encoded = None
    for piece in pieces_of(node_hidden[...], 2):
        term = dot(embed_out_t[...], piece)
        encoded = term if encoded is None else encoded + term
    mesh_in[...] = encoded
    mean_sq = jnp.mean(encoded * encoded, axis=0, keepdims=True)
    gain = lanes(gain_t[...], M_DEV)
    normed[...] = (encoded * lax.rsqrt(mean_sq + 1e-05) * gain).astype(BF16)

    normed_flights = []
    for chunk in range(4):
        nodes = pl.ds(128 * chunk, 128)
        normed_flights.append(
            copies.start(
                normed_in.at[:, pl.ds(256 * chunk, 256)],
                [
                    (normed.at[:, nodes], normed_in.at[:, pl.ds(256 * chunk + 128 * slot, 128)], device)
                    for side, device, slot in sides
                ],
            )
        )

    target_flights += [send_target(512 * chunk, 512) for chunk in range(2, 4)]

    loads["qkv"].wait()
    q_t[...] = jnp.transpose(qkv_ref[0])
    k_t[...] = jnp.transpose(qkv_ref[1])
    v_t[...] = jnp.transpose(qkv_ref[2])
    unit_q[...] = unit_heads(dot(q_t[...], normed[...]), M_DEV).astype(BF16)

    loads["head_scale"].wait()
    score_scale = head_scale_ref[...] / HEAD_DIM

    def attend(near, start, width):
        keys = unit_heads(dot(k_t[...], near), width).astype(BF16)
        unit_k[start : start + width, :] = jnp.transpose(keys)
        values[:, start : start + width] = dot(v_t[...], near).astype(BF16)
        sums_now = []
        count = counts[start : start + width, :]
        for head in range(HEADS):
            part = slice(HEAD_DIM * head, HEAD_DIM * head + HEAD_DIM)
            scores = dot(unit_k[start : start + width, part], unit_q[part, :])
            exp = jnp.exp(scores * score_scale[:, head : head + 1])
            exps[head, start : start + width, :] = exp
            sums_now.append(jnp.sum(exp * count, axis=0, keepdims=True))
        return sums_now

    loads["nbr"].wait()
    window = nbr_ref[...] - (base - M_DEV)
    patch = lax.shift_right_arithmetic(window, jnp.full_like(window, 9))
    within[...] = window - patch * M_DEV
    fields[...] = jnp.where(patch == 0, 64, jnp.where(patch == 1, 1, 4096))

    @pl.loop(0, 8)
    def _(block):
        ids = lax.broadcasted_iota(I32, (64, M_DEV), 0) + block * 64
        total = jnp.zeros((64, M_DEV), I32)
        for j in range(NBR):
            total = total + jnp.where(within[j : j + 1, :] == ids, fields[j : j + 1, :], 0)
        chunk = block // 2
        part = (block - 2 * chunk) * 64
        for start, shift in (
            (block * 64, 0),
            (M_DEV + 256 * chunk + part, 6),
            (M_DEV + 256 * chunk + 128 + part, 12),
        ):
            count = lax.shift_right_logical(total, jnp.full_like(total, shift)) & 63
            rows = pl.ds(pl.multiple_of(start, 64), 64)
            counts[rows, :] = count.astype(F32)
            counts_16[rows, :] = count.astype(F32).astype(BF16)

    cell_flight.wait_recv()
    for slot in range(2):
        prepare(1 + slot, m2g_in[slot])

    loads["out_w"].wait()
    loads["dec_w"].wait()
    out_t[...] = jnp.transpose(out_w_ref[...])
    dec_t[...] = jnp.zeros_like(dec_t)
    dec_t[:VARS, :] = dec_w_ref[...]
    dec_full[...] = jnp.transpose(dec_t[...])
    exp_sums = None
    for chunk in range(6):
        if chunk < 2:
            near = normed[:, 256 * chunk : 256 * chunk + 256]
        else:
            normed_flights[chunk - 2].wait_recv()
            near = normed_in[:, 256 * (chunk - 2) : 256 * (chunk - 2) + 256]
        sums_now = attend(near, 256 * chunk, 256)
        exp_sums = sums_now if exp_sums is None else [a + b for a, b in zip(exp_sums, sums_now)]

    for head in range(HEADS):
        inverse = 1.0 / exp_sums[head]
        part = slice(HEAD_DIM * head, HEAD_DIM * head + HEAD_DIM)

        probs[head] = (exps[head] * inverse).astype(BF16) * counts_16[...]
        attended[part, :] = dot(values[part, :], probs[head]).astype(BF16)

    mesh_out[...] = (mesh_in[...] + dot(out_t[...], attended[...])).astype(BF16)
    for index, piece in enumerate(pieces_of(dot(dec_t[:ROWS, :], mesh_out[...]), 2)):
        vars_two[ROWS * index : ROWS * index + ROWS, :] = piece
    scale_all = 1.0 / (MEMBERS * VARS)
    grad_scale = 2.0 * out_scale * scale_all
    grad_net[VARS:, :] = jnp.zeros((ROWS - VARS, 3 * G_DEV), BF16)
    loss_row = jnp.zeros((1, 512), F32)
    sources = ((noisy_ref, target_ref), (state_in.at[0], target_in.at[0]), (state_in.at[1], target_in.at[1]))
    chunks = [(0, chunk) for chunk in range(4)] + [(place, chunk) for chunk in range(4) for place in (1, 2)]
    for place, chunk in chunks:
        state, target = sources[place]
        if place == 1 and chunk == 0:
            target_flights[0].wait_recv()
            target_flights[1].wait_recv()
        if place == 1 and chunk == 2:
            target_flights[2].wait_recv()
            target_flights[3].wait_recv()
        cells = slice(512 * chunk, 512 * chunk + 512)
        block = slice(G_DEV * place + 512 * chunk, G_DEV * place + 512 * chunk + 512)
        both = dot(vars_two[...], table[:, block])
        net = both[:VARS, :] + both[ROWS : ROWS + VARS, :]
        weights = weights_ref[:, block]
        errors = skip_scale * state[:, cells].astype(F32) + out_scale * net - target[:, cells].astype(F32)
        weighted = weights * errors
        loss_row = loss_row + jnp.sum(weighted * errors, axis=0, keepdims=True)
        grad_net[:VARS, block] = (grad_scale * weights * errors).astype(BF16)
    loss = jnp.sum(loss_row, axis=1, keepdims=True) * scale_all
    node_grad = dot(grad_net[...], table_t[...])
    node_pieces = pieces_of(node_grad, 2)
    grown = None
    for piece in node_pieces:
        term = dot(dec_full[:, :ROWS], piece)
        grown = term if grown is None else grown + term
    mesh_grad[...] = grown.astype(BF16)

    units = []
    for index, unit in enumerate(UNITS):
        units.append(
            device_sum(parts[unit[0]], totals[unit[3]], unit, unit_refs[7 * index : 7 * index + 7], copies, at)
        )
    out_units, value_units = (units[:3], units[3:])
    out_sum = dot_t(attended[...], mesh_grad[...])
    for lane in range(4):
        part_out[512 * lane : 512 * lane + 512, :] = out_sum[:, 128 * lane : 128 * lane + 128]
    for unit in out_units[:2]:
        next(unit)
    head_grad[...] = dot(out_w_ref[...], mesh_grad[...]).astype(BF16)
    dec_sum = None
    for piece in node_pieces:
        term = dot_t(piece, mesh_out[...])
        dec_sum = term if dec_sum is None else dec_sum + term
    for lane in range(4):
        start = 2048 + ROWS * lane
        part_out[start : start + ROWS, :] = dec_sum[:, 128 * lane : 128 * lane + 128]
    part_out[2048 + 4 * ROWS :, :] = jnp.broadcast_to(loss, (128, 128))
    next(out_units[2])
    def advance(some):
        for unit in some:
            next(unit)

    for pair in range(2):
        spread = jnp.concatenate(
            [
                dot_t(head_grad[HEAD_DIM * head : HEAD_DIM * head + HEAD_DIM, :], probs[head]).astype(BF16)
                for head in (2 * pair, 2 * pair + 1)
            ],
            axis=0,
        )
        both = dot_t(normed[...], spread[:, :M_DEV]) + dot_t(normed_in[...], spread[:, M_DEV:])
        for index in range(2):
            start = 1024 * pair + 512 * index
            part_value[start : start + 512, :] = both[:, HEAD_DIM * index : HEAD_DIM * index + HEAD_DIM]
        if pair == 0:
            next(value_units[0])
            advance(out_units)
    advance(value_units[1:])
    next(value_units[0])
    order = ((value_units[1:],),) + ((out_units, value_units),) * 6
    for groups in order:
        for group in groups:
            advance(group)
    assert [next(unit, "end") for unit in units] == ["end"] * len(units)
    for copy in copies.all:
        copy.wait_send()


def finish_kernel(out_a, out_b, value_a, value_b, out_hbm, value_hbm, dec_result, loss_result, sems):
    flights = []
    for index, (source, tail, target) in enumerate(((out_a, out_b, out_hbm), (value_a, value_b, value_hbm))):
        for lane in range(4):
            flights.append(
                pltpu.make_async_copy(
                    source.at[pl.ds(512 * lane, 512), :] if lane < 3 else tail.at[pl.ds(0, 512), :],
                    target.at[:, pl.ds(128 * lane, 128)],
                    sems.at[4 * index + lane],
                )
            )
            flights[-1].start()
    for lane in range(4):
        start = 512 + ROWS * lane
        dec_result[:, 128 * lane : 128 * lane + 128] = out_b[start : start + VARS, :]
    loss_result[...] = out_b[512 + 4 * ROWS : 513 + 4 * ROWS, :1] / GRID
    for flight in flights:
        flight.wait()


def local(
    noisy_state,
    target_state,
    noise_level,
    var_weight,
    embed_in,
    embed_out,
    norm_gain,
    qkv_weight,
    head_scale,
    out_weight,
    dec_weight,
    g2m_node,
    m2g_node,
    neighbours,
):
    vmem = pl.BlockSpec(memory_space=pltpu.VMEM)
    anywhere = pl.BlockSpec(memory_space=pl.ANY)
    copies = 15 + 8 * len(UNITS)
    scratch = [pltpu.SemaphoreType.DMA((copies,))] * 2 + [pltpu.SemaphoreType.DMA((len(INPUTS),))]
    scratch += [pltpu.VMEM(entry[-2], entry[-1]) for entry in INPUTS + SCRATCH]
    for unit in UNITS:
        scratch += sum_scratch(unit[2])
    totals = pl.pallas_call(
        step_kernel,
        out_shape=[pltpu.VMEM(shape, F32) for shape in TOTALS],
        in_specs=[anywhere] * len(INPUTS),
        out_specs=[vmem] * len(TOTALS),
        scratch_shapes=scratch,
        compiler_params=pltpu.CompilerParams(
            collective_id=0, has_side_effects=True, vmem_limit_bytes=STEP_VMEM
        ),
        name="step",
    )(
        noisy_state,
        g2m_node.reshape(1, G_DEV),
        embed_in,
        embed_out,
        norm_gain.reshape(1, D),
        qkv_weight,
        neighbours.T,
        m2g_node.reshape(1, G_DEV),
        out_weight,
        dec_weight.T,
        target_state,
        var_weight.reshape(1, VARS),
        noise_level.reshape(1, 1),
        head_scale.reshape(1, HEADS),
    )
    square = jax.ShapeDtypeStruct((D, D), F32)
    grad_out, grad_value, dec, loss = pl.pallas_call(
        finish_kernel,
        out_shape=(square, square, jax.ShapeDtypeStruct((VARS, D), F32), jax.ShapeDtypeStruct((1, 1), F32)),
        in_specs=[vmem] * len(TOTALS),
        out_specs=(anywhere, anywhere, vmem, vmem),
        scratch_shapes=[pltpu.SemaphoreType.DMA((8,))],
        compiler_params=pltpu.CompilerParams(vmem_limit_bytes=8 << 20),
        name="finish",
    )(*[total.reshape(-1, 128) for total in totals])
    return loss.reshape(()), dec.T, grad_out, grad_value


def solution(mesh):
    in_specs = (
        P(("chan", "member"), None, "band"),
        P(("chan", "member"), None, "band"),
        P(("chan", "member")),
        P(),
        P(),
        P(),
        P(),
        P(),
        P(),
        P(),
        P(),
        P("band"),
        P("band"),
        P("band", None),
    )
    out_specs = (P(), P(), P(), P())
    return jax.shard_map(local, mesh=mesh, in_specs=in_specs, out_specs=out_specs, check_vma=False)
```
